32 devices in a mesh: groups: 2 (over y), rowt: 4 (over z), colt: 2 (over x), site: 2 (over core).
Axes of the slice: x: 2, y: 2, z: 4, core: 2. Of those that a mesh axis runs over, the one named last changes fastest.
Arguments:
- seed_green: bfloat16 [8, 2, 768, 768], P(('groups', 'rowt'), 'colt', None, 'site'), parts along dimension 0, may hold values from -6 to 6
- field_spins: int32 [4, 8, 768], P(None, ('groups', 'rowt')), parts along dimension 1, may hold values from 0 to 1
- hop_matrix: float32 [768, 768], replicated, may hold values from -0.21875 to 0.21875
- vertex: bfloat16 [768, 768], replicated, may hold values from -0.21875 to 0.21875
Outputs:
- measured: bfloat16 [8, 2, 768, 768], P(('groups', 'rowt'), 'colt', None, 'site'), parts along dimension 0
The draws below stay inside these ranges and needn't reach their ends.
There are 2 independent parts, one for each index of `groups`. The reference program is written for one: setup_inputs(seed, part) draws one part's arguments, and reference() takes and returns one part's arrays. A program takes and returns all parts, laid end to end along the dimension named above; an argument that names none is the same for every part. Nothing has to cross between parts.
All inputs are finite; a program needn't handle non-finite values.
Results may differ from the reference program's by a relative error of at most 0.0051.
Values may be sent and summed in bfloat16 or wider, within the bound.
No kernel may reach another device: no remote copies, remote signals or barrier semaphores. Data moves between devices by JAX's collectives and lax.ppermute only.
A program may use at most 64 MiB of HBM per device.

```python
import jax
import jax.numpy as jnp
from jax import lax

N = 768
WRAPS = 4
TR = 4
TC = 2


def set_ends(result, rng, smallest, top_value):
    shape = result.shape
    spot = [jax.random.randint(jax.random.fold_in(rng, axis), (), 0, shape[axis]) for axis in range(len(shape))]
    result = result.at[tuple(spot)].set(smallest)
    longest = shape.index(max(shape))
    spot[longest] = (spot[longest] + 1) % shape[longest]
    return result.at[tuple(spot)].set(top_value)


def block_scale(own_key, dims, cuts, least, largest):
    def one(position, shards_of):
        steps = jax.random.uniform(jax.random.fold_in(jax.random.fold_in(own_key, 6), position), (shards_of,), jnp.float32, least / len(cuts), largest / len(cuts))
        return jnp.repeat(jnp.exp(steps), dims[position] // shards_of).reshape((-1,) + (1,) * (len(dims) - position - 1))

    loudness = one(*cuts[0])
    for cut in cuts[1:]:
        loudness = loudness * one(*cut)
    return loudness


def normal_values(own_key, extent, scale, bound, cuts=(), held_as=jnp.bfloat16):
    factor_of = block_scale(own_key, extent, cuts, -0.22, 0.18) if cuts else 1.0
    entries = jax.random.normal(own_key, extent, jnp.float32) * scale * factor_of
    return jnp.minimum(jnp.maximum(entries, -bound), bound).astype(held_as)


def setup_inputs(seed: int = 0, part: int = 0) -> dict:
    arg_keys = jax.random.split(jax.random.key(seed), 5)
    part_keys = jax.random.split(jax.random.fold_in(arg_keys[4], part), 5)
    seed_green = normal_values(part_keys[0], (TR, TC, N, N), 1.0, 6.0, ((0, 4), (1, 2), (3, 2)))
    field_spins = set_ends(jax.random.randint(part_keys[1], (WRAPS, TR, N), 0, 2), jax.random.fold_in(part_keys[1], 1), 0, 1).astype(jnp.int32)
    hop_matrix = normal_values(arg_keys[2], (N, N), N ** -0.5, 0.21875, (), jnp.float32)
    vertex = normal_values(arg_keys[3], (N, N), N ** -0.5, 0.21875)
    return {"seed_green": seed_green, "field_spins": field_spins, "hop_matrix": hop_matrix, "vertex": vertex}


coupling = 0.45
keep_share = 0.8
hop_share = 0.3


def reference(seed_green, field_spins, hop_matrix, vertex):
    row_count = seed_green.shape[0]
    col_count = seed_green.shape[1]
    weights = jnp.exp(coupling * (2.0 * field_spins.astype(jnp.float32) - 1.0))
    vertex_wide = vertex.astype(jnp.float32)

    def one_row(row_index):
        current = lax.dynamic_index_in_dim(seed_green, row_index, 0, keepdims=False).astype(jnp.float32)
        measured = jnp.zeros_like(current)
        for wrap_step in range(WRAPS):
            target = (row_index + wrap_step + 1) % row_count
            weights_row = lax.dynamic_index_in_dim(weights[wrap_step], target, 0, keepdims=False)
            sign_value = jnp.where(target == 0, -1.0, 1.0).astype(jnp.float32)
            hopped = jnp.einsum("ab,cbd->cad", hop_matrix, current, precision=lax.Precision.HIGHEST)
            image = keep_share * current + hop_share * hopped
            current = (sign_value * weights_row)[None, :, None] * image
            rounded = current.astype(jnp.bfloat16)
            partner = jnp.roll(rounded, col_count // 2, axis=0)
            pair_product = (rounded.astype(jnp.float32) * jnp.swapaxes(partner, 1, 2).astype(jnp.float32)).astype(jnp.bfloat16)
            measured = measured + jnp.einsum("ab,cbd->cad", vertex_wide, pair_product.astype(jnp.float32))
        return (measured / WRAPS).astype(jnp.bfloat16)

    return lax.map(one_row, jnp.arange(row_count, dtype=jnp.int32))
```

```python
import functools

import jax
import jax.numpy as jnp
from jax import lax
from jax.experimental import pallas as pl
from jax.experimental.pallas import tpu as pltpu
from jax.sharding import PartitionSpec as P

coupling = 0.45
keep_share = 0.8
hop_share = 0.3
LANES = 128


def split_halves(value):
    high = value.astype(jnp.bfloat16)
    low = (value - high.astype(jnp.float32)).astype(jnp.bfloat16)
    return high, low


def own_kernel(row_count, seed_ref, hop_ref, *refs):
    wraps = len(refs) - 5
    spin_refs = refs[:wraps]
    turned_out, hop_out, scale_out, high_t, low_t = refs[wraps:]
    row_index = lax.axis_index("rowt")
    scaled = hop_share * hop_ref[...]
    high, low = split_halves(scaled)
    hop_out[...] = high
    high_t[...] = high.T
    low_t[...] = low.T
    turned = seed_ref[...].T.astype(jnp.float32)
    scales = []
    for step in range(wraps):
        spins = spin_refs[step][...].astype(jnp.float32)
        sign = jnp.where((row_index + step + 1) % row_count == 0, -1.0, 1.0)
        scales.append(sign * jnp.exp(coupling * (2.0 * spins - 1.0)))
    for step in range(wraps):
        column = jnp.broadcast_to(scales[step], (8, scales[step].shape[1])).T[:, :1]
        scale_out[step] = jnp.broadcast_to(column, scale_out.shape[1:])
        turned_high, turned_low = split_halves(turned)
        hopped = jnp.dot(turned_high, high_t[...], preferred_element_type=jnp.float32)
        hopped += jnp.dot(turned_high, low_t[...], preferred_element_type=jnp.float32)
        if step:
            hopped += jnp.dot(turned_low, high_t[...], preferred_element_type=jnp.float32)
        turned = scales[step] * (keep_share * turned + hopped)
        turned_out[step] = turned.astype(jnp.bfloat16)


def pair_kernel(offset, first, last, *refs):
    ours, theirs, turned_ref, hop_ref, scale_ref, vertex_ref = refs[:6]
    total_ref = None if first else refs[6]
    out_ref, level = refs[-2:]
    wraps, width, sites = turned_ref.shape
    part = ours.shape[1]
    site = lax.axis_index("site")
    rows = pl.ds(pl.multiple_of(site * width, LANES), width)
    spots = [
        pl.ds(pl.multiple_of(place * width + offset, LANES), part)
        for place in (site, lax.axis_size("site") - 1 - site)
    ]
    level[...] = jnp.concatenate([ours[...], theirs[...]], axis=1).astype(jnp.float32)
    copies = 2 * part // LANES
    pairs = None
    for step in range(wraps):
        narrow = level[...].astype(jnp.bfloat16)
        if step < wraps - 1:
            hopped = jnp.dot(hop_ref[...], narrow, preferred_element_type=jnp.float32)
            scale = jnp.concatenate([scale_ref[step]] * copies, axis=1)
            level[...] = scale * (keep_share * level[...] + hopped)
            met = level[rows, :]
        else:
            hopped = jnp.dot(hop_ref[rows, :], narrow, preferred_element_type=jnp.float32)
            scale = jnp.concatenate([scale_ref[step, rows, :]] * copies, axis=1)
            met = scale * (keep_share * level[rows, :] + hopped)
        met = met.astype(jnp.bfloat16).astype(jnp.float32)
        own = jnp.concatenate([turned_ref[step, :, spot] for spot in spots], axis=1)
        product = (met * own.astype(jnp.float32)).astype(jnp.bfloat16).astype(jnp.float32)
        pairs = product if pairs is None else pairs + product
    corner = jnp.concatenate([vertex_ref[:, spot] for spot in spots], axis=1)
    total = 0.0 if first else total_ref[...]
    for half in split_halves(pairs):
        total = total + lax.dot_general(
            corner, half, (((1,), (1,)), ((), ())), preferred_element_type=jnp.float32
        )
    if last:
        total = total / wraps
    out_ref[...] = total.astype(out_ref.dtype)


def per_device(seed_green, field_spins, hop_matrix, vertex):
    wraps = field_spins.shape[0]
    rows, cols, sites = (lax.axis_size(name) for name in ("rowt", "colt", "site"))
    seed = seed_green[0, 0]
    sites_n, width = seed.shape
    vmem = pl.BlockSpec(memory_space=pltpu.VMEM)

    cut = width - LANES if width > LANES else width
    spans = [(start, stop) for start, stop in ((0, cut), (cut, width)) if stop > start]
    across = [(i, (i + cols // 2) % cols) for i in range(cols)]
    swap = [(i, sites - 1 - i) for i in range(sites)]
    arrived = [lax.ppermute(seed[:, a:b], "colt", across) for a, b in spans]
    swapped = [lax.ppermute(piece, "site", swap) for piece in arrived]

    spins = field_spins[:, 0, :].astype(jnp.bfloat16)
    needed = []
    for step in range(wraps):
        line = spins[step : step + 1]
        shift = (step + 1) % rows
        if shift:
            line = lax.ppermute(line, "rowt", [((i + shift) % rows, i) for i in range(rows)])
        needed.append(line)

    flops = 2 * sites_n * sites_n * width
    turned, hop, scale = pl.pallas_call(
        functools.partial(own_kernel, rows),
        out_shape=(
            jax.ShapeDtypeStruct((wraps, width, sites_n), jnp.bfloat16),
            jax.ShapeDtypeStruct((sites_n, sites_n), jnp.bfloat16),
            jax.ShapeDtypeStruct((wraps, sites_n, LANES), jnp.float32),
        ),
        in_specs=[vmem] * (2 + wraps),
        out_specs=(vmem,) * 3,
        scratch_shapes=[pltpu.VMEM((sites_n, sites_n), jnp.bfloat16)] * 2,
        compiler_params=pltpu.CompilerParams(vmem_limit_bytes=24 << 20),
        cost_estimate=pl.CostEstimate(flops=11 * flops, bytes_accessed=1 << 22, transcendentals=0),
        name="own",
    )(seed, hop_matrix, *needed)

    total = None
    for number, (start, stop) in enumerate(spans):
        last = number == len(spans) - 1
        operands = [arrived[number], swapped[number], turned, hop, scale, vertex]
        if number:
            operands.append(total)
        total = pl.pallas_call(
            functools.partial(pair_kernel, start, number == 0, last),
            out_shape=jax.ShapeDtypeStruct(
                (sites_n, width), jnp.bfloat16 if last else jnp.float32
            ),
            in_specs=[vmem] * len(operands),
            out_specs=vmem,
            scratch_shapes=[pltpu.VMEM((sites_n, 2 * (stop - start)), jnp.float32)],
            compiler_params=pltpu.CompilerParams(vmem_limit_bytes=24 << 20),
            cost_estimate=pl.CostEstimate(
                flops=8 * flops * (stop - start) // width, bytes_accessed=1 << 22, transcendentals=0
            ),
            name=f"pair{number}",
        )(*operands)
    return total[None, None]


def solution(mesh):
    return jax.shard_map(
        per_device,
        mesh=mesh,
        in_specs=(
            P(("groups", "rowt"), "colt", None, "site"),
            P(None, ("groups", "rowt"), None),
            P(),
            P(),
        ),
        out_specs=P(("groups", "rowt"), "colt", None, "site"),
        check_vma=False,
    )
```

```python
import functools

import jax
import jax.numpy as jnp
from jax import lax
from jax.experimental import pallas as pl
from jax.experimental.pallas import tpu as pltpu
from jax.sharding import PartitionSpec as P


coupling = 0.45
keep_share = 0.8
hop_share = 0.3
LANES = 128


VMEM = pl.BlockSpec(memory_space=pltpu.VMEM)
HBM = pl.BlockSpec(memory_space=pltpu.HBM)


def limit(mebibytes):
    return pltpu.CompilerParams(vmem_limit_bytes=mebibytes << 20)


def in_hbm(array):
    return pltpu.with_memory_space_constraint(array, pltpu.HBM)


def split_halves(value):
    high = value.astype(jnp.bfloat16)
    low = (value - high.astype(jnp.float32)).astype(jnp.bfloat16)
    return high, low


def cut_kernel(spans, seed_ref, spins_ref, *refs):
    pieces, lines = refs[: len(spans)], refs[len(spans) : -3]
    spins_in, piece_sems, spin_sem = refs[-3:]
    spin_copy = pltpu.make_async_copy(spins_ref, spins_in, spin_sem)
    copies = [
        pltpu.make_async_copy(seed_ref.at[:, pl.ds(a, b - a)], piece, piece_sems.at[number])
        for number, ((a, b), piece) in enumerate(zip(spans, pieces))
    ]
    for copy in copies:
        copy.start()
    spin_copy.start()
    spin_copy.wait()
    for step, line in enumerate(lines):
        line[...] = spins_in[step].astype(jnp.float32).astype(jnp.bfloat16)
    for copy in copies:
        copy.wait()


def prepare_kernel(hop_ref, *refs):
    pieces = refs[:-4]
    hop_out, high_t, low_t, turned_out = refs[-4:]
    start = 0
    for piece in pieces:
        turned_out[start : start + piece.shape[1], :] = piece[...].T
        start += piece.shape[1]
    for start in range(0, hop_ref.shape[0], LANES):
        span = slice(start, start + LANES)
        high, low = split_halves(hop_share * hop_ref[span, :])
        hop_out[span, :] = high
        high_t[:, span] = high.T
        low_t[:, span] = low.T


def own_kernel(row_count, seed_t, high_t, low_t, *refs):
    wraps = len(refs) - 2
    turned_out, scale_out = refs[wraps:]
    row_index = lax.axis_index("rowt")
    turned = seed_t[...].astype(jnp.float32)
    narrow = seed_t[...]
    for step in range(wraps):
        spins = refs[step][...].astype(jnp.float32)
        sign = jnp.where((row_index + step + 1) % row_count == 0, -1.0, 1.0)
        scale = sign * jnp.exp(coupling * (2.0 * spins - 1.0))
        column = jnp.broadcast_to(scale, (8, scale.shape[1])).T[:, :1]
        scale_out[step] = jnp.broadcast_to(column, scale_out.shape[1:])
        hopped = jnp.dot(narrow, high_t[...], preferred_element_type=jnp.float32)
        hopped += jnp.dot(narrow, low_t[...], preferred_element_type=jnp.float32)
        turned = scale * (keep_share * turned + hopped)
        narrow = turned.astype(jnp.bfloat16)
        turned_out[step] = narrow


def site_spans(width):
    site = lax.axis_index("site")
    places = (site, lax.axis_size("site") - 1 - site)
    return [pl.ds(pl.multiple_of(place * width, LANES), width) for place in places]


def advance(step, spans, hop_ref, scale_ref, level, narrow):
    source, target = step % 2, (step + 1) % 2
    copies = level.shape[1] // LANES
    for span in spans:
        hopped = jnp.dot(hop_ref[span, :], narrow[source], preferred_element_type=jnp.float32)
        scale = jnp.concatenate([scale_ref[step, span, :]] * copies, axis=1)
        moved = scale * (keep_share * level[span, :] + hopped)
        rounded = moved.astype(jnp.bfloat16)
        level[span, :] = moved
        narrow[target, span, :] = rounded
        yield rounded


def chain_kernel(arrived, hop_ref, scale_ref, keep_out, send_out, level, narrow):
    spans = site_spans(keep_out.shape[1])
    narrow[0] = arrived[...]
    level[...] = arrived[...].astype(jnp.float32)
    for step in range(keep_out.shape[0]):
        rounded = advance(step, spans, hop_ref, scale_ref, level, narrow)
        for out, value in zip((keep_out, send_out), rounded):
            out[step] = value


def multiply(met, own):
    product = met.astype(jnp.float32) * own.astype(jnp.float32)
    return product.astype(jnp.bfloat16).astype(jnp.float32)


def columns_at(offset, part, width):
    site = lax.axis_index("site")
    places = (site, lax.axis_size("site") - 1 - site)
    return [pl.ds(pl.multiple_of(place * width + offset, LANES), part) for place in places]


def sum_kernel(offset, ours, theirs, turned_ref, vertex_ref, out_ref):
    wraps, width, _ = turned_ref.shape
    total = None
    for met_ref, spot in zip((ours, theirs), columns_at(offset, ours.shape[2], width)):
        pairs = None
        for step in range(wraps):
            product = multiply(met_ref[step], turned_ref[step, :, spot])
            pairs = product if pairs is None else pairs + product
        for half in split_halves(pairs):
            part = lax.dot_general(
                vertex_ref[:, spot],
                half,
                (((1,), (1,)), ((), ())),
                preferred_element_type=jnp.float32,
            )
            total = part if total is None else total + part
    out_ref[...] = total


def finish_kernel(offset, *refs):
    ours, theirs, turned_ref, hop_ref, scale_ref, vertex_ref, total_ref = refs[:7]
    out_ref, level, narrow, result, sems = refs[7:]
    wraps, width, sites = turned_ref.shape
    spans = site_spans(width)
    spots = columns_at(offset, ours.shape[1], width)
    arrived = jnp.concatenate([ours[...], theirs[...]], axis=1)
    narrow[0] = arrived
    level[...] = arrived.astype(jnp.float32)
    pairs = None
    for step in range(wraps):
        needed = spans if step < wraps - 1 else spans[:1]
        met = list(advance(step, needed, hop_ref, scale_ref, level, narrow))[0]
        own = jnp.concatenate([turned_ref[step, :, spot] for spot in spots], axis=1)
        product = multiply(met, own)
        pairs = product if pairs is None else pairs + product
    halves = split_halves(pairs)
    blocks = sems.shape[0]
    size = sites // blocks
    copies = []
    for block in range(blocks):
        span = slice(block * size, (block + 1) * size)
        corner = jnp.concatenate([vertex_ref[span, spot] for spot in spots], axis=1)
        total = total_ref[span, :]
        for half in halves:
            total = total + lax.dot_general(
                corner, half, (((1,), (1,)), ((), ())), preferred_element_type=jnp.float32
            )
        result[span, :] = (total / wraps).astype(result.dtype)
        copy = pltpu.make_async_copy(
            result.at[pl.ds(block * size, size)],
            out_ref.at[pl.ds(block * size, size)],
            sems.at[block],
        )
        copy.start()
        copies.append(copy)
    for copy in copies:
        copy.wait()


def cut(seed, spins, spans):
    wraps, sites = spins.shape[0], seed.shape[0]
    outs = [jax.ShapeDtypeStruct((sites, b - a), jnp.bfloat16) for a, b in spans]
    outs += [jax.ShapeDtypeStruct((1, sites), jnp.bfloat16)] * wraps
    result = pl.pallas_call(
        functools.partial(cut_kernel, spans),
        out_shape=outs,
        in_specs=[HBM, HBM],
        out_specs=[VMEM] * len(outs),
        scratch_shapes=[
            pltpu.VMEM(spins.shape, spins.dtype),
            pltpu.SemaphoreType.DMA((len(spans),)),
            pltpu.SemaphoreType.DMA,
        ],
        compiler_params=limit(8),
        name="cut",
    )(in_hbm(seed), in_hbm(spins))
    return result[: len(spans)], result[len(spans) :]


def prepare(hop_matrix, pieces):
    sites = hop_matrix.shape[0]
    width = sum(piece.shape[1] for piece in pieces)
    square = jax.ShapeDtypeStruct((sites, sites), jnp.bfloat16)
    return pl.pallas_call(
        prepare_kernel,
        out_shape=[square] * 3 + [jax.ShapeDtypeStruct((width, sites), jnp.bfloat16)],
        in_specs=[VMEM] * (1 + len(pieces)),
        out_specs=[VMEM] * 4,
        compiler_params=limit(8),
        cost_estimate=pl.CostEstimate(flops=1 << 28, bytes_accessed=1 << 22, transcendentals=0),
        name="prepare",
    )(hop_matrix, *pieces)


def propagate(row_count, seed_t, high_t, low_t, lines):
    width, sites = seed_t.shape
    wraps = len(lines)
    return pl.pallas_call(
        functools.partial(own_kernel, row_count),
        out_shape=[
            jax.ShapeDtypeStruct((wraps, width, sites), jnp.bfloat16),
            jax.ShapeDtypeStruct((wraps, sites, LANES), jnp.float32),
        ],
        in_specs=[VMEM] * (3 + wraps),
        out_specs=[VMEM] * 2,
        compiler_params=limit(16),
        cost_estimate=pl.CostEstimate(
            flops=4 * wraps * sites * sites * width, bytes_accessed=1 << 22, transcendentals=0
        ),
        name="propagate",
    )(seed_t, high_t, low_t, *lines)


def work(columns, sites, wraps):
    return pl.CostEstimate(
        flops=2 * wraps * sites * sites * columns, bytes_accessed=1 << 22, transcendentals=0
    )


def levels(sites, columns):
    return [
        pltpu.VMEM((sites, columns), jnp.float32),
        pltpu.VMEM((2, sites, columns), jnp.bfloat16),
    ]


def chain(arrived, hop, scale, width):
    sites, columns = arrived.shape
    wraps = scale.shape[0]
    shape = jax.ShapeDtypeStruct((wraps, width, columns), jnp.bfloat16)
    return pl.pallas_call(
        chain_kernel,
        out_shape=[shape] * 2,
        in_specs=[VMEM] * 3,
        out_specs=[VMEM] * 2,
        scratch_shapes=levels(sites, columns),
        compiler_params=limit(16),
        cost_estimate=work(columns, sites, wraps),
        name="chain",
    )(arrived, hop, scale)


def add_up(offset, ours, theirs, turned, vertex):
    _, width, sites = turned.shape
    return pl.pallas_call(
        functools.partial(sum_kernel, offset),
        out_shape=jax.ShapeDtypeStruct((sites, width), jnp.float32),
        in_specs=[VMEM] * 4,
        out_specs=VMEM,
        compiler_params=limit(16),
        cost_estimate=work(ours.shape[2], sites, 2),
        name="add_up",
    )(ours, theirs, turned, vertex)


def finish(offset, *operands):
    ours, turned = operands[0], operands[2]
    wraps, width, sites = turned.shape
    blocks = 4
    return pl.pallas_call(
        functools.partial(finish_kernel, offset),
        out_shape=jax.ShapeDtypeStruct((sites, width), jnp.bfloat16),
        in_specs=[VMEM] * len(operands),
        out_specs=HBM,
        scratch_shapes=levels(sites, 2 * ours.shape[1])
        + [pltpu.VMEM((sites, width), jnp.bfloat16), pltpu.SemaphoreType.DMA((blocks,))],
        compiler_params=limit(16),
        cost_estimate=work(2 * ours.shape[1], sites, wraps),
        name="finish",
    )(*operands)


def fetch_lines(spins):
    rows, count = lax.axis_size("rowt"), len(spins)
    lines = [None] * count
    if rows == count and rows & (rows - 1) == 0:
        index = lax.axis_index("rowt")
        every = jnp.concatenate(spins, axis=0)
        for bits in range(1, rows):
            back = (index - (index ^ bits)) % rows
            line = lax.dynamic_slice_in_dim(every, back - 1, 1, 0)
            lines[bits - 1] = lax.ppermute(line, "rowt", [(i, i ^ bits) for i in range(rows)])
        came = jnp.concatenate(lines[:-1] + [spins[-1]], axis=0)
        ordered = [
            lax.dynamic_slice_in_dim(came, (index ^ (index + w) % rows) - 1, 1, 0)
            for w in range(1, rows)
        ]
        return ordered + [spins[-1]]
    for step, line in enumerate(spins):
        shift = (step + 1) % rows
        if shift:
            line = lax.ppermute(line, "rowt", [((i + shift) % rows, i) for i in range(rows)])
        lines[step] = line
    return lines


def per_device(seed_green, field_spins, hop_matrix, vertex):
    cols, sites = lax.axis_size("colt"), lax.axis_size("site")
    width = seed_green.shape[-1]
    edge = width - LANES
    across = [(i, (i + cols // 2) % cols) for i in range(cols)]
    swap = [(i, sites - 1 - i) for i in range(sites)]

    pieces, spins = cut(seed_green[0, 0], field_spins, [(0, edge), (edge, width)])
    first = lax.ppermute(pieces[0], "colt", across)
    second = lax.ppermute(pieces[1], "colt", across)
    lines = fetch_lines(spins)
    hop, high_t, low_t, seed_t = prepare(hop_matrix, pieces)
    turned, scale = propagate(lax.axis_size("rowt"), seed_t, high_t, low_t, lines)
    keep, send = chain(first, hop, scale, width)
    came = lax.ppermute(send, "site", swap)
    other = lax.ppermute(second, "site", swap)
    total = add_up(0, keep, came, turned, vertex)
    result = finish(edge, second, other, turned, hop, scale, vertex, total)
    return result[None, None]


def solution(mesh):
    return jax.shard_map(
        per_device,
        mesh=mesh,
        in_specs=(
            P(("groups", "rowt"), "colt", None, "site"),
            P(None, ("groups", "rowt"), None),
            P(),
            P(),
        ),
        out_specs=P(("groups", "rowt"), "colt", None, "site"),
        check_vma=False,
    )
```

```python
import functools

import jax
import jax.numpy as jnp
from jax import lax
from jax.experimental import pallas as pl
from jax.experimental.pallas import tpu as pltpu
from jax.sharding import PartitionSpec as P


coupling = 0.45
keep_share = 0.8
hop_share = 0.3
LANES = 128


VMEM = pl.BlockSpec(memory_space=pltpu.VMEM)
HBM = pl.BlockSpec(memory_space=pltpu.HBM)


def limit(mebibytes):
    return pltpu.CompilerParams(vmem_limit_bytes=mebibytes << 20)


def in_hbm(array):
    return pltpu.with_memory_space_constraint(array, pltpu.HBM)


def split_halves(value):
    high = value.astype(jnp.bfloat16)
    low = (value - high.astype(jnp.float32)).astype(jnp.bfloat16)
    return high, low


def site_spans(width):
    site = lax.axis_index("site")
    places = (site, lax.axis_size("site") - 1 - site)
    return [pl.ds(pl.multiple_of(place * width, LANES), width) for place in places]


def cut_kernel(spans, seed_ref, spins_ref, *refs):
    pieces, lines = refs[: len(spans)], refs[len(spans)]
    spins_in, piece_sems, spin_sem = refs[-3:]
    width = seed_ref.shape[1]
    sources = site_spans(width)
    copies = []
    for (a, b), piece in zip(spans, pieces):
        for half, source in enumerate(sources):
            copy = pltpu.make_async_copy(
                seed_ref.at[source, pl.ds(a, b - a)],
                piece.at[pl.ds(half * width, width)],
                piece_sems.at[len(copies)],
            )
            copy.start()
            copies.append(copy)
    spin_copy = pltpu.make_async_copy(spins_ref, spins_in, spin_sem)
    spin_copy.start()
    spin_copy.wait()
    parts = []
    for step in range(lines.shape[0]):
        parts.append(
            jnp.concatenate([spins_in[step, :, source] for source in sources], axis=1)
        )
    lines[...] = jnp.concatenate(parts, axis=0).astype(jnp.float32).astype(jnp.bfloat16)
    for copy in copies:
        copy.wait()


def hold_kernel(lines_ref, out_ref):
    out_ref[...] = lines_ref[...]


def prepare_kernel(hop_ref, *refs):
    pieces = refs[:-4]
    hop_out, high_t, low_t, turned_out = refs[-4:]
    width, _ = turned_out.shape
    start = 0
    for piece in pieces:
        turned_out[start : start + piece.shape[1], :] = piece[...].T
        start += piece.shape[1]
    site = lax.axis_index("site")
    places = (site, lax.axis_size("site") - 1 - site)
    for half, place in enumerate(places):
        for start in range(0, width, LANES):
            rows = pl.ds(pl.multiple_of(place * width + start, LANES), LANES)
            strip = jnp.concatenate([hop_ref[rows, span] for span in site_spans(width)], axis=1)
            high, low = split_halves(hop_share * strip)
            spot = slice(half * width + start, half * width + start + LANES)
            hop_out[spot, :] = high
            high_t[:, spot] = high.T
            low_t[:, spot] = low.T


def hop_turned(narrow, high_t, low_t):
    hopped = jnp.dot(narrow, high_t[...], preferred_element_type=jnp.float32)
    return hopped + jnp.dot(narrow, low_t[...], preferred_element_type=jnp.float32)


def lift_kernel(seed_t, high_t, low_t, image_out):
    narrow = seed_t[...]
    hopped = hop_turned(narrow, high_t, low_t)
    image_out[...] = keep_share * narrow.astype(jnp.float32) + hopped


def own_kernel(row_count, image_ref, high_t, low_t, *refs):
    wraps = len(refs) - 2
    turned_out, scale_out = refs[wraps:]
    row_index = lax.axis_index("rowt")
    image = image_ref[...]
    for step in range(wraps):
        spins = refs[step][...].astype(jnp.float32)
        sign = jnp.where((row_index + step + 1) % row_count == 0, -1.0, 1.0)
        scale = sign * jnp.exp(coupling * (2.0 * spins - 1.0))
        column = jnp.broadcast_to(scale, (8, scale.shape[1])).T[:, :1]
        scale_out[step] = jnp.broadcast_to(column, scale_out.shape[1:])
        turned = scale * image
        narrow = turned.astype(jnp.bfloat16)
        turned_out[step] = narrow
        if step < wraps - 1:
            image = keep_share * turned + hop_turned(narrow, high_t, low_t)


def advance(step, spans, hop_ref, scale_ref, level, narrow):
    source, target = step % 2, (step + 1) % 2
    copies = level.shape[1] // LANES
    for span in spans:
        hopped = jnp.dot(hop_ref[span, :], narrow[source], preferred_element_type=jnp.float32)
        scale = jnp.concatenate([scale_ref[step, span, :]] * copies, axis=1)
        moved = scale * (keep_share * level[span, :] + hopped)
        rounded = moved.astype(jnp.bfloat16)
        level[span, :] = moved
        narrow[target, span, :] = rounded
        yield rounded


def chain_kernel(arrived, hop_ref, scale_ref, keep_out, send_out, level, narrow):
    width = keep_out.shape[1]
    spans = [slice(0, width), slice(width, 2 * width)]
    narrow[0] = arrived[...]
    level[...] = arrived[...].astype(jnp.float32)
    for step in range(keep_out.shape[0]):
        rounded = advance(step, spans, hop_ref, scale_ref, level, narrow)
        for out, value in zip((keep_out, send_out), rounded):
            out[step] = value


def multiply(met, own):
    product = met.astype(jnp.float32) * own.astype(jnp.float32)
    return product.astype(jnp.bfloat16).astype(jnp.float32)


def columns_at(offset, part, width):
    site = lax.axis_index("site")
    places = (site, lax.axis_size("site") - 1 - site)
    held = [slice(offset, offset + part), slice(width + offset, width + offset + part)]
    return held, [pl.ds(pl.multiple_of(p * width + offset, LANES), part) for p in places]


def sum_kernel(offset, ours, theirs, turned_ref, vertex_ref, out_ref):
    wraps, width, _ = turned_ref.shape
    total = None
    for met_ref, held, spot in zip((ours, theirs), *columns_at(offset, ours.shape[2], width)):
        pairs = None
        for step in range(wraps):
            product = multiply(met_ref[step], turned_ref[step, :, held])
            pairs = product if pairs is None else pairs + product
        for half in split_halves(pairs):
            part = lax.dot_general(
                vertex_ref[:, spot],
                half,
                (((1,), (1,)), ((), ())),
                preferred_element_type=jnp.float32,
            )
            total = part if total is None else total + part
    out_ref[...] = total


def finish_kernel(offset, *refs):
    ours, theirs, turned_ref, hop_ref, scale_ref, vertex_ref, total_ref = refs[:7]
    out_ref, level, narrow, result, sems = refs[7:]
    wraps, width, sites = turned_ref.shape
    spans = [slice(0, width), slice(width, 2 * width)]
    held, spots = columns_at(offset, ours.shape[1], width)
    other = jnp.concatenate([theirs[span, :] for span in reversed(spans)], axis=0)
    arrived = jnp.concatenate([ours[...], other], axis=1)
    narrow[0] = arrived
    level[...] = arrived.astype(jnp.float32)
    pairs = None
    for step in range(wraps):
        needed = spans if step < wraps - 1 else spans[:1]
        met = list(advance(step, needed, hop_ref, scale_ref, level, narrow))[0]
        own = jnp.concatenate([turned_ref[step, :, span] for span in held], axis=1)
        product = multiply(met, own)
        pairs = product if pairs is None else pairs + product
    halves = split_halves(pairs)
    blocks = sems.shape[0]
    size = sites // blocks
    copies = []
    for block in range(blocks):
        span = slice(block * size, (block + 1) * size)
        corner = jnp.concatenate([vertex_ref[span, spot] for spot in spots], axis=1)
        total = total_ref[span, :]
        for half in halves:
            total = total + lax.dot_general(
                corner, half, (((1,), (1,)), ((), ())), preferred_element_type=jnp.float32
            )
        result[span, :] = (total / wraps).astype(result.dtype)
        copy = pltpu.make_async_copy(
            result.at[pl.ds(block * size, size)],
            out_ref.at[pl.ds(block * size, size)],
            sems.at[block],
        )
        copy.start()
        copies.append(copy)
    for copy in copies:
        copy.wait()


def cut(seed, spins, spans):
    wraps, sites = spins.shape[0], seed.shape[0]
    outs = [jax.ShapeDtypeStruct((sites, b - a), jnp.bfloat16) for a, b in spans]
    outs.append(jax.ShapeDtypeStruct((wraps, sites), jnp.bfloat16))
    *pieces, lines = pl.pallas_call(
        functools.partial(cut_kernel, spans),
        out_shape=outs,
        in_specs=[HBM, HBM],
        out_specs=[VMEM] * len(outs),
        scratch_shapes=[
            pltpu.VMEM(spins.shape, spins.dtype),
            pltpu.SemaphoreType.DMA((2 * len(spans),)),
            pltpu.SemaphoreType.DMA,
        ],
        compiler_params=limit(8),
        name="cut",
    )(in_hbm(seed), in_hbm(spins))
    return pieces, lines


def hold(lines):
    return pl.pallas_call(
        hold_kernel,
        out_shape=jax.ShapeDtypeStruct(lines.shape, lines.dtype),
        in_specs=[VMEM],
        out_specs=VMEM,
        compiler_params=limit(4),
        cost_estimate=pl.CostEstimate(flops=1 << 32, bytes_accessed=1 << 24, transcendentals=0),
        name="hold",
    )(lines)


def prepare(hop_matrix, pieces):
    sites = hop_matrix.shape[0]
    width = sum(piece.shape[1] for piece in pieces)
    square = jax.ShapeDtypeStruct((sites, sites), jnp.bfloat16)
    return pl.pallas_call(
        prepare_kernel,
        out_shape=[square] * 3 + [jax.ShapeDtypeStruct((width, sites), jnp.bfloat16)],
        in_specs=[VMEM] * (1 + len(pieces)),
        out_specs=[VMEM] * 4,
        compiler_params=limit(8),
        cost_estimate=pl.CostEstimate(flops=1 << 28, bytes_accessed=1 << 22, transcendentals=0),
        name="prepare",
    )(hop_matrix, *pieces)


def lift(seed_t, high_t, low_t):
    width, sites = seed_t.shape
    return pl.pallas_call(
        lift_kernel,
        out_shape=jax.ShapeDtypeStruct((width, sites), jnp.float32),
        in_specs=[VMEM] * 3,
        out_specs=VMEM,
        compiler_params=limit(16),
        cost_estimate=work(width, sites, 2),
        name="lift",
    )(seed_t, high_t, low_t)


def propagate(row_count, image, high_t, low_t, lines):
    width, sites = image.shape
    wraps = len(lines)
    return pl.pallas_call(
        functools.partial(own_kernel, row_count),
        out_shape=[
            jax.ShapeDtypeStruct((wraps, width, sites), jnp.bfloat16),
            jax.ShapeDtypeStruct((wraps, sites, LANES), jnp.float32),
        ],
        in_specs=[VMEM] * (3 + wraps),
        out_specs=[VMEM] * 2,
        compiler_params=limit(16),
        cost_estimate=work(width, sites, 2 * (wraps - 1)),
        name="propagate",
    )(image, high_t, low_t, *lines)


def work(columns, sites, wraps):
    return pl.CostEstimate(
        flops=2 * wraps * sites * sites * columns, bytes_accessed=1 << 22, transcendentals=0
    )


def levels(sites, columns):
    return [
        pltpu.VMEM((sites, columns), jnp.float32),
        pltpu.VMEM((2, sites, columns), jnp.bfloat16),
    ]


def chain(arrived, hop, scale, width):
    sites, columns = arrived.shape
    wraps = scale.shape[0]
    shape = jax.ShapeDtypeStruct((wraps, width, columns), jnp.bfloat16)
    return pl.pallas_call(
        chain_kernel,
        out_shape=[shape] * 2,
        in_specs=[VMEM] * 3,
        out_specs=[VMEM] * 2,
        scratch_shapes=levels(sites, columns),
        compiler_params=limit(16),
        cost_estimate=work(columns, sites, wraps),
        name="chain",
    )(arrived, hop, scale)


def add_up(offset, ours, theirs, turned, vertex):
    _, width, sites = turned.shape
    return pl.pallas_call(
        functools.partial(sum_kernel, offset),
        out_shape=jax.ShapeDtypeStruct((sites, width), jnp.float32),
        in_specs=[VMEM] * 4,
        out_specs=VMEM,
        compiler_params=limit(16),
        cost_estimate=work(ours.shape[2], sites, 2),
        name="add_up",
    )(ours, theirs, turned, vertex)


def finish(offset, *operands):
    ours, turned = operands[0], operands[2]
    wraps, width, sites = turned.shape
    blocks = 2
    return pl.pallas_call(
        functools.partial(finish_kernel, offset),
        out_shape=jax.ShapeDtypeStruct((sites, width), jnp.bfloat16),
        in_specs=[VMEM] * len(operands),
        out_specs=HBM,
        scratch_shapes=levels(sites, 2 * ours.shape[1])
        + [pltpu.VMEM((sites, width), jnp.bfloat16), pltpu.SemaphoreType.DMA((blocks,))],
        compiler_params=limit(16),
        cost_estimate=work(2 * ours.shape[1], sites, wraps),
        name="finish",
    )(*operands)


def fetch_lines(lines):
    rows, count = lax.axis_size("rowt"), lines.shape[0]
    if rows == count and rows & (rows - 1) == 0:
        bit = 1
        while bit < rows:
            came = lax.ppermute(lines, "rowt", [(i, i ^ bit) for i in range(rows)])
            lines = jnp.concatenate([lines, came], axis=0)
            bit *= 2
        index = lax.axis_index("rowt")
        picks = [(index ^ (index + w) % rows) * count + w - 1 for w in range(1, rows)]
        found = [lax.dynamic_slice_in_dim(lines, pick, 1, 0) for pick in picks]
        return found + [lines[count - 1 : count]]
    found = []
    for step in range(count):
        line, shift = lines[step : step + 1], (step + 1) % rows
        if shift:
            line = lax.ppermute(line, "rowt", [((i + shift) % rows, i) for i in range(rows)])
        found.append(line)
    return found


def per_device(seed_green, field_spins, hop_matrix, vertex):
    cols, sites = lax.axis_size("colt"), lax.axis_size("site")
    width = seed_green.shape[-1]
    edge = width - LANES
    across = [(i, (i + cols // 2) % cols) for i in range(cols)]
    swap = [(i, sites - 1 - i) for i in range(sites)]

    pieces, lines = cut(seed_green[0, 0], field_spins, [(0, edge), (edge, width)])
    first = lax.ppermute(pieces[0], "colt", across)
    second = lax.ppermute(pieces[1], "colt", across)
    lines = fetch_lines(hold(lines))
    hop, high_t, low_t, seed_t = prepare(hop_matrix, pieces)
    image = lift(seed_t, high_t, low_t)
    turned, scale = propagate(lax.axis_size("rowt"), image, high_t, low_t, lines)
    keep, send = chain(first, hop, scale, width)
    came = lax.ppermute(send, "site", swap)
    other = lax.ppermute(second, "site", swap)
    total = add_up(0, keep, came, turned, vertex)
    result = finish(edge, second, other, turned, hop, scale, vertex, total)
    return result[None, None]


def solution(mesh):
    return jax.shard_map(
        per_device,
        mesh=mesh,
        in_specs=(
            P(("groups", "rowt"), "colt", None, "site"),
            P(None, ("groups", "rowt"), None),
            P(),
            P(),
        ),
        out_specs=P(("groups", "rowt"), "colt", None, "site"),
        check_vma=False,
    )
```

```python
import functools

import jax
import jax.numpy as jnp
from jax import lax
from jax.experimental import pallas as pl
from jax.experimental.pallas import tpu as pltpu
from jax.sharding import PartitionSpec as P


coupling = 0.45
keep_share = 0.8
hop_share = 0.3
LANES = 128


VMEM = pl.BlockSpec(memory_space=pltpu.VMEM)
HBM = pl.BlockSpec(memory_space=pltpu.HBM)


def limit(mebibytes):
    return pltpu.CompilerParams(vmem_limit_bytes=mebibytes << 20)


def in_hbm(array):
    return pltpu.with_memory_space_constraint(array, pltpu.HBM)


def split_halves(value):
    high = value.astype(jnp.bfloat16)
    low = (value - high.astype(jnp.float32)).astype(jnp.bfloat16)
    return high, low


def site_spans(width):
    site = lax.axis_index("site")
    places = (site, lax.axis_size("site") - 1 - site)
    return [pl.ds(pl.multiple_of(place * width, LANES), width) for place in places]


def cut_kernel(spans, seed_ref, spins_ref, *refs):
    pieces, lines = refs[: len(spans)], refs[len(spans)]
    spins_in, piece_sems, spin_sem = refs[-3:]
    width = seed_ref.shape[1]
    sources = site_spans(width)
    copies = []
    for (a, b), piece in zip(spans, pieces):
        for half, source in enumerate(sources):
            copy = pltpu.make_async_copy(
                seed_ref.at[source, pl.ds(a, b - a)],
                piece.at[pl.ds(half * width, width)],
                piece_sems.at[len(copies)],
            )
            copy.start()
            copies.append(copy)
    spin_copy = pltpu.make_async_copy(spins_ref, spins_in, spin_sem)
    spin_copy.start()
    spin_copy.wait()
    parts = []
    for step in range(lines.shape[0]):
        parts.append(
            jnp.concatenate([spins_in[step, :, source] for source in sources], axis=1)
        )
    lines[...] = jnp.concatenate(parts, axis=0).astype(jnp.float32).astype(jnp.bfloat16)
    for copy in copies:
        copy.wait()


def hold_kernel(lines_ref, out_ref):
    out_ref[...] = lines_ref[...]


def prepare_kernel(hop_ref, *refs):
    pieces = refs[:-4]
    hop_out, high_t, low_t, turned_out = refs[-4:]
    width, _ = turned_out.shape
    start = 0
    for piece in pieces:
        turned_out[start : start + piece.shape[1], :] = piece[...].T
        start += piece.shape[1]
    site = lax.axis_index("site")
    places = (site, lax.axis_size("site") - 1 - site)
    for half, place in enumerate(places):
        for start in range(0, width, LANES):
            rows = pl.ds(pl.multiple_of(place * width + start, LANES), LANES)
            strip = jnp.concatenate([hop_ref[rows, span] for span in site_spans(width)], axis=1)
            high, low = split_halves(hop_share * strip)
            spot = slice(half * width + start, half * width + start + LANES)
            hop_out[spot, :] = high
            high_t[:, spot] = high.T
            low_t[:, spot] = low.T


def hop_turned(narrow, high_t, low_t):
    hopped = jnp.dot(narrow, high_t[...], preferred_element_type=jnp.float32)
    return hopped + jnp.dot(narrow, low_t[...], preferred_element_type=jnp.float32)


def lift_kernel(seed_t, high_t, low_t, image_out):
    narrow = seed_t[...]
    hopped = hop_turned(narrow, high_t, low_t)
    image_out[...] = keep_share * narrow.astype(jnp.float32) + hopped


def join_kernel(held_ref, came_ref, out_ref):
    out_ref[...] = jnp.concatenate([held_ref[...], came_ref[...]], axis=0)


def weigh_kernel(row_count, doubled, *refs):
    *line_refs, scale_out, column_out = refs
    wraps = scale_out.shape[0]
    row_index = lax.axis_index("rowt")
    lines = jnp.concatenate([ref[...].astype(jnp.float32) for ref in line_refs], axis=0)
    places = lax.broadcasted_iota(jnp.int32, lines.shape, 0)
    scales = []
    for step in range(wraps):
        target = (row_index + step + 1) % row_count
        if doubled:
            pick = (row_index ^ target) * wraps + step
            spins = jnp.sum(jnp.where(places == pick, lines, 0.0), axis=0, keepdims=True)
        else:
            spins = lines[step : step + 1]
        sign = jnp.where(target == 0, -1.0, 1.0)
        scales.append(sign * jnp.exp(coupling * (2.0 * spins - 1.0)))
    scale = jnp.concatenate(scales, axis=0)
    scale_out[...] = scale
    columns = scale.T
    for step in range(wraps):
        column_out[step] = jnp.broadcast_to(columns[:, step : step + 1], column_out.shape[1:])


def own_kernel(first, image_ref, high_t, low_t, scale_ref, turned_out, *rest):
    steps, total = turned_out.shape[0], scale_ref.shape[0]
    image = image_ref[...]
    for step in range(steps):
        turned = scale_ref[first + step : first + step + 1, :] * image
        narrow = turned.astype(jnp.bfloat16)
        turned_out[step] = narrow
        if first + step < total - 1:
            image = keep_share * turned + hop_turned(narrow, high_t, low_t)
    if rest:
        rest[0][...] = image


def advance(step, spans, hop_ref, scale_ref, level, narrow):
    source, target = step % 2, (step + 1) % 2
    copies = level.shape[1] // LANES
    for span in spans:
        hopped = jnp.dot(hop_ref[span, :], narrow[source], preferred_element_type=jnp.float32)
        scale = jnp.concatenate([scale_ref[step, span, :]] * copies, axis=1)
        moved = scale * (keep_share * level[span, :] + hopped)
        rounded = moved.astype(jnp.bfloat16)
        level[span, :] = moved
        narrow[target, span, :] = rounded
        yield rounded


def chain_kernel(arrived, hop_ref, scale_ref, keep_out, send_out, level, narrow):
    width = keep_out.shape[1]
    spans = [slice(0, width), slice(width, 2 * width)]
    narrow[0] = arrived[...]
    level[...] = arrived[...].astype(jnp.float32)
    for step in range(keep_out.shape[0]):
        rounded = advance(step, spans, hop_ref, scale_ref, level, narrow)
        for out, value in zip((keep_out, send_out), rounded):
            out[step] = value


def multiply(met, own):
    return (met * own).astype(jnp.float32)


def own_levels(turned_refs, spans):
    for turned_ref in turned_refs:
        for step in range(turned_ref.shape[0]):
            parts = [turned_ref[step, :, span] for span in spans]
            yield parts[0] if len(parts) == 1 else jnp.concatenate(parts, axis=1)


def columns_at(offset, part, width):
    site = lax.axis_index("site")
    places = (site, lax.axis_size("site") - 1 - site)
    held = [slice(offset, offset + part), slice(width + offset, width + offset + part)]
    return held, [pl.ds(pl.multiple_of(p * width + offset, LANES), part) for p in places]


def sum_kernel(offset, ours, theirs, *refs):
    *turned_refs, vertex_ref, out_ref = refs
    width = ours.shape[1]
    total = None
    for met_ref, held, spot in zip((ours, theirs), *columns_at(offset, ours.shape[2], width)):
        pairs = None
        for step, own in enumerate(own_levels(turned_refs, [held])):
            product = multiply(met_ref[step], own)
            pairs = product if pairs is None else pairs + product
        for half in split_halves(pairs):
            part = lax.dot_general(
                vertex_ref[:, spot],
                half,
                (((1,), (1,)), ((), ())),
                preferred_element_type=jnp.float32,
            )
            total = part if total is None else total + part
    out_ref[...] = total


def finish_kernel(offset, *refs):
    ours, theirs, hop_ref, scale_ref, vertex_ref, total_ref, *turned_refs = refs[:-5]
    out_ref, level, narrow, result, sems = refs[-5:]
    wraps, (sites, width) = scale_ref.shape[0], total_ref.shape
    spans = [slice(0, width), slice(width, 2 * width)]
    held, spots = columns_at(offset, ours.shape[1], width)
    other = jnp.concatenate([theirs[span, :] for span in reversed(spans)], axis=0)
    arrived = jnp.concatenate([ours[...], other], axis=1)
    narrow[0] = arrived
    level[...] = arrived.astype(jnp.float32)
    pairs = None
    for step, own in enumerate(own_levels(turned_refs, held)):
        needed = spans if step < wraps - 1 else spans[:1]
        met = list(advance(step, needed, hop_ref, scale_ref, level, narrow))[0]
        product = multiply(met, own)
        pairs = product if pairs is None else pairs + product
    halves = split_halves(pairs)
    blocks = sems.shape[0]
    size = sites // blocks
    copies = []
    for block in range(blocks):
        span = slice(block * size, (block + 1) * size)
        corner = jnp.concatenate([vertex_ref[span, spot] for spot in spots], axis=1)
        total = total_ref[span, :]
        for half in halves:
            total = total + lax.dot_general(
                corner, half, (((1,), (1,)), ((), ())), preferred_element_type=jnp.float32
            )
        result[span, :] = (total / wraps).astype(result.dtype)
        copy = pltpu.make_async_copy(
            result.at[pl.ds(block * size, size)],
            out_ref.at[pl.ds(block * size, size)],
            sems.at[block],
        )
        copy.start()
        copies.append(copy)
    for copy in copies:
        copy.wait()


def cut(seed, spins, spans):
    wraps, sites = spins.shape[0], seed.shape[0]
    outs = [jax.ShapeDtypeStruct((sites, b - a), jnp.bfloat16) for a, b in spans]
    outs.append(jax.ShapeDtypeStruct((wraps, sites), jnp.bfloat16))
    *pieces, lines = pl.pallas_call(
        functools.partial(cut_kernel, spans),
        out_shape=outs,
        in_specs=[HBM, HBM],
        out_specs=[VMEM] * len(outs),
        scratch_shapes=[
            pltpu.VMEM(spins.shape, spins.dtype),
            pltpu.SemaphoreType.DMA((2 * len(spans),)),
            pltpu.SemaphoreType.DMA,
        ],
        compiler_params=limit(8),
        name="cut",
    )(in_hbm(seed), in_hbm(spins))
    return pieces, lines


def hold(lines):
    return pl.pallas_call(
        hold_kernel,
        out_shape=jax.ShapeDtypeStruct(lines.shape, lines.dtype),
        in_specs=[VMEM],
        out_specs=VMEM,
        compiler_params=limit(4),
        cost_estimate=pl.CostEstimate(flops=1 << 32, bytes_accessed=1 << 24, transcendentals=0),
        name="hold",
    )(lines)


def prepare(hop_matrix, pieces):
    sites = hop_matrix.shape[0]
    width = sum(piece.shape[1] for piece in pieces)
    square = jax.ShapeDtypeStruct((sites, sites), jnp.bfloat16)
    return pl.pallas_call(
        prepare_kernel,
        out_shape=[square] * 3 + [jax.ShapeDtypeStruct((width, sites), jnp.bfloat16)],
        in_specs=[VMEM] * (1 + len(pieces)),
        out_specs=[VMEM] * 4,
        compiler_params=limit(8),
        cost_estimate=pl.CostEstimate(flops=1 << 28, bytes_accessed=1 << 22, transcendentals=0),
        name="prepare",
    )(hop_matrix, *pieces)


def lift(seed_t, high_t, low_t):
    width, sites = seed_t.shape
    return pl.pallas_call(
        lift_kernel,
        out_shape=jax.ShapeDtypeStruct((width, sites), jnp.float32),
        in_specs=[VMEM] * 3,
        out_specs=VMEM,
        compiler_params=limit(16),
        cost_estimate=work(width, sites, 2),
        name="lift",
    )(seed_t, high_t, low_t)


def join(held, came):
    shape = (held.shape[0] + came.shape[0], held.shape[1])
    return pl.pallas_call(
        join_kernel,
        out_shape=jax.ShapeDtypeStruct(shape, held.dtype),
        in_specs=[VMEM] * 2,
        out_specs=VMEM,
        compiler_params=limit(4),
        name="join",
    )(held, came)


def weigh(wraps, lines, doubled):
    sites = lines[0].shape[1]
    return pl.pallas_call(
        functools.partial(weigh_kernel, lax.axis_size("rowt"), doubled),
        out_shape=[
            jax.ShapeDtypeStruct((wraps, sites), jnp.float32),
            jax.ShapeDtypeStruct((wraps, sites, LANES), jnp.float32),
        ],
        in_specs=[VMEM] * len(lines),
        out_specs=[VMEM] * 2,
        compiler_params=limit(8),
        name="weigh",
    )(*lines)


def propagate(first, last, image, high_t, low_t, scale):
    width, sites = image.shape
    wraps, steps = scale.shape[0], last - first
    outs = [jax.ShapeDtypeStruct((steps, width, sites), jnp.bfloat16)]
    if last < wraps:
        outs.append(jax.ShapeDtypeStruct((width, sites), jnp.float32))
    return pl.pallas_call(
        functools.partial(own_kernel, first),
        out_shape=outs,
        in_specs=[VMEM] * 4,
        out_specs=[VMEM] * len(outs),
        compiler_params=limit(16),
        cost_estimate=work(width, sites, 2 * steps),
        name="late" if first else "early",
    )(image, high_t, low_t, scale)


def work(columns, sites, wraps):
    return pl.CostEstimate(
        flops=2 * wraps * sites * sites * columns, bytes_accessed=1 << 22, transcendentals=0
    )


def levels(sites, columns):
    return [
        pltpu.VMEM((sites, columns), jnp.float32),
        pltpu.VMEM((2, sites, columns), jnp.bfloat16),
    ]


def chain(arrived, hop, scale, width):
    sites, columns = arrived.shape
    wraps = scale.shape[0]
    shape = jax.ShapeDtypeStruct((wraps, width, columns), jnp.bfloat16)
    return pl.pallas_call(
        chain_kernel,
        out_shape=[shape] * 2,
        in_specs=[VMEM] * 3,
        out_specs=[VMEM] * 2,
        scratch_shapes=levels(sites, columns),
        compiler_params=limit(16),
        cost_estimate=work(columns, sites, wraps),
        name="chain",
    )(arrived, hop, scale)


def add_up(offset, ours, theirs, turned, vertex):
    _, width, columns = ours.shape
    sites = vertex.shape[0]
    return pl.pallas_call(
        functools.partial(sum_kernel, offset),
        out_shape=jax.ShapeDtypeStruct((sites, width), jnp.float32),
        in_specs=[VMEM] * (3 + len(turned)),
        out_specs=VMEM,
        compiler_params=limit(16),
        cost_estimate=work(columns, sites, 2),
        name="add_up",
    )(ours, theirs, *turned, vertex)


def finish(offset, ours, theirs, hop, columns, vertex, total, turned):
    sites, width = total.shape
    blocks = 2
    return pl.pallas_call(
        functools.partial(finish_kernel, offset),
        out_shape=jax.ShapeDtypeStruct((sites, width), jnp.bfloat16),
        in_specs=[VMEM] * (6 + len(turned)),
        out_specs=HBM,
        scratch_shapes=levels(sites, 2 * ours.shape[1])
        + [pltpu.VMEM((sites, width), jnp.bfloat16), pltpu.SemaphoreType.DMA((blocks,))],
        compiler_params=limit(16),
        cost_estimate=work(2 * ours.shape[1], sites, columns.shape[0]),
        name="finish",
    )(ours, theirs, hop, columns, vertex, total, *turned)


def fetch_lines(lines):
    rows, count = lax.axis_size("rowt"), lines.shape[0]
    if rows == count and rows & (rows - 1) == 0:
        bit = 1
        while bit < rows:
            came = lax.ppermute(lines, "rowt", [(i, i ^ bit) for i in range(rows)])
            bit *= 2
            if bit < rows:
                lines = join(lines, came)
        return [lines, came], True
    found = []
    for step in range(count):
        line, shift = lines[step : step + 1], (step + 1) % rows
        if shift:
            line = lax.ppermute(line, "rowt", [((i + shift) % rows, i) for i in range(rows)])
        found.append(line)
    return found, False


def per_device(seed_green, field_spins, hop_matrix, vertex):
    cols, sites = lax.axis_size("colt"), lax.axis_size("site")
    wraps, width = field_spins.shape[0], seed_green.shape[-1]
    edge = width - LANES
    across = [(i, (i + cols // 2) % cols) for i in range(cols)]
    swap = [(i, sites - 1 - i) for i in range(sites)]

    pieces, lines = cut(seed_green[0, 0], field_spins, [(0, edge), (edge, width)])
    first = lax.ppermute(pieces[0], "colt", across)
    second = lax.ppermute(pieces[1], "colt", across)
    found, doubled = fetch_lines(hold(lines))
    hop, high_t, low_t, seed_t = prepare(hop_matrix, pieces)
    image = lift(seed_t, high_t, low_t)
    scale, columns = weigh(wraps, found, doubled)
    keep, send = chain(first, hop, columns, width)
    came = lax.ppermute(send, "site", swap)
    middle = wraps // 2
    early, image = propagate(0, middle, image, high_t, low_t, scale)
    other = lax.ppermute(second, "site", swap)
    (late,) = propagate(middle, wraps, image, high_t, low_t, scale)
    turned = [early, late]
    total = add_up(0, keep, came, turned, vertex)
    result = finish(edge, second, other, hop, columns, vertex, total, turned)
    return result[None, None]


def solution(mesh):
    return jax.shard_map(
        per_device,
        mesh=mesh,
        in_specs=(
            P(("groups", "rowt"), "colt", None, "site"),
            P(None, ("groups", "rowt"), None),
            P(),
            P(),
        ),
        out_specs=P(("groups", "rowt"), "colt", None, "site"),
        check_vma=False,
    )
```

```python
import functools

import jax
import jax.numpy as jnp
from jax import lax
from jax.experimental import pallas as pl
from jax.experimental.pallas import tpu as pltpu
from jax.sharding import PartitionSpec as P


coupling = 0.45
keep_share = 0.8
hop_share = 0.3
LANES = 128
PIECES = 4


VMEM = pl.BlockSpec(memory_space=pltpu.VMEM)
HBM = pl.BlockSpec(memory_space=pltpu.HBM)


def limit(mebibytes):
    return pltpu.CompilerParams(vmem_limit_bytes=mebibytes << 20)


def in_hbm(array):
    return pltpu.with_memory_space_constraint(array, pltpu.HBM)


def split_halves(value):
    high = value.astype(jnp.bfloat16)
    low = (value - high.astype(jnp.float32)).astype(jnp.bfloat16)
    return high, low


def site_spans(width):
    site = lax.axis_index("site")
    places = (site, lax.axis_size("site") - 1 - site)
    return [pl.ds(pl.multiple_of(place * width, LANES), width) for place in places]


def cut_kernel(spans, seed_ref, spins_ref, *refs):
    pieces, lines = refs[: len(spans)], refs[len(spans)]
    spins_in, piece_sems, spin_sem = refs[-3:]
    width = seed_ref.shape[1]
    sources = site_spans(width)
    copies = []
    for (a, b), piece in zip(spans, pieces):
        for half, source in enumerate(sources):
            copy = pltpu.make_async_copy(
                seed_ref.at[source, pl.ds(a, b - a)],
                piece.at[pl.ds(half * width, width)],
                piece_sems.at[len(copies)],
            )
            copy.start()
            copies.append(copy)
    spin_copy = pltpu.make_async_copy(spins_ref, spins_in, spin_sem)
    spin_copy.start()
    spin_copy.wait()
    parts = []
    for step in range(lines.shape[0]):
        parts.append(
            jnp.concatenate([spins_in[step, :, source] for source in sources], axis=1)
        )
    lines[...] = jnp.concatenate(parts, axis=0).astype(jnp.float32).astype(jnp.bfloat16)
    for copy in copies:
        copy.wait()


def hold_kernel(lines_ref, out_ref):
    out_ref[...] = lines_ref[...]


def prepare_kernel(hop_ref, *refs):
    pieces = refs[:-4]
    hop_out, high_t, low_t, turned_out = refs[-4:]
    width, _ = turned_out.shape
    start = 0
    for piece in pieces:
        turned_out[start : start + piece.shape[1], :] = piece[...].T
        start += piece.shape[1]
    site = lax.axis_index("site")
    places = (site, lax.axis_size("site") - 1 - site)
    for half, place in enumerate(places):
        for start in range(0, width, LANES):
            rows = pl.ds(pl.multiple_of(place * width + start, LANES), LANES)
            strip = jnp.concatenate([hop_ref[rows, span] for span in site_spans(width)], axis=1)
            high, low = split_halves(hop_share * strip)
            spot = slice(half * width + start, half * width + start + LANES)
            hop_out[spot, :] = high
            high_t[:, spot] = high.T
            low_t[:, spot] = low.T


def hop_turned(narrow, high_t, low_t):
    hopped = jnp.dot(narrow, high_t[...], preferred_element_type=jnp.float32)
    if low_t is not None:
        hopped += jnp.dot(narrow, low_t[...], preferred_element_type=jnp.float32)
    return hopped


def lift_kernel(seed_t, high_t, low_t, _, image_out):
    narrow = seed_t[...]
    hopped = hop_turned(narrow, high_t, low_t)
    image_out[...] = keep_share * narrow.astype(jnp.float32) + hopped


def join_kernel(held_ref, came_ref, out_ref):
    out_ref[...] = jnp.concatenate([held_ref[...], came_ref[...]], axis=0)


def early_kernel(row_count, doubled, image_ref, high_t, low_t, *refs):
    *line_refs, turned_out, image_out, scale_out, column_out = refs
    wraps = scale_out.shape[0]
    row_index = lax.axis_index("rowt")
    lines = jnp.concatenate([ref[...].astype(jnp.float32) for ref in line_refs], axis=0)
    places = lax.broadcasted_iota(jnp.int32, lines.shape, 0)
    scales = []
    for step in range(wraps):
        target = (row_index + step + 1) % row_count
        if doubled:
            pick = (row_index ^ target) * wraps + step
            spins = jnp.sum(jnp.where(places == pick, lines, 0.0), axis=0, keepdims=True)
        else:
            spins = lines[step : step + 1]
        sign = jnp.where(target == 0, -1.0, 1.0)
        scales.append(sign * jnp.exp(coupling * (2.0 * spins - 1.0)))
    turned = scales[0] * image_ref[...]
    narrow = turned.astype(jnp.bfloat16)
    turned_out[0] = narrow
    image_out[...] = keep_share * turned + hop_turned(narrow, high_t, low_t)
    scale = jnp.concatenate(scales, axis=0)
    scale_out[...] = scale
    columns = scale.T
    for step in range(wraps):
        column_out[step] = jnp.broadcast_to(columns[:, step : step + 1], column_out.shape[1:])


def own_kernel(first, image_ref, high_t, low_t, scale_ref, turned_out, *rest):
    steps, total = turned_out.shape[0], scale_ref.shape[0]
    image = image_ref[...]
    for step in range(steps):
        turned = scale_ref[first + step : first + step + 1, :] * image
        narrow = turned.astype(jnp.bfloat16)
        turned_out[step] = narrow
        if first + step < total - 1:
            low = low_t if first + step < total - 2 else None
            image = keep_share * turned + hop_turned(narrow, high_t, low)
    if rest:
        rest[0][...] = image


def spread(columns, pieces):
    size = columns.shape[0] // pieces
    starts = range(0, columns.shape[0], size)
    return [columns[start : start + size].astype(jnp.float32) for start in starts]


def advance(step, halves, hop_ref, scale_ref, level, narrow):
    size, copies = level[0].shape[0], level[0].shape[1] // LANES
    source = jnp.concatenate(narrow, axis=0)
    new, fresh = [], []
    each = len(level) // 2
    for half in range(halves):
        for number in range(half * each, half * each + each):
            span = slice(number * size, (number + 1) * size)
            hopped = jnp.dot(hop_ref[span, :], source, preferred_element_type=jnp.float32)
            scale = jnp.concatenate([scale_ref[step, span, :]] * copies, axis=1)
            moved = scale * (keep_share * level[number] + hopped)
            new.append(moved)
            fresh.append(moved.astype(jnp.bfloat16))
        yield jnp.concatenate(fresh[half * each : half * each + each], axis=0)
    if halves == 2:
        level[:], narrow[:] = new, fresh


def chain_kernel(arrived, hop_ref, scale_ref, keep_out, send_out):
    level = spread(arrived[...], PIECES)
    narrow = [block.astype(jnp.bfloat16) for block in level]
    for step in range(keep_out.shape[0]):
        rounded = advance(step, 2, hop_ref, scale_ref, level, narrow)
        for value, out in zip(rounded, (keep_out, send_out)):
            out[step] = value


def multiply(met, own):
    return (met * own).astype(jnp.float32)


def own_levels(turned_refs, spans):
    for turned_ref in turned_refs:
        for step in range(turned_ref.shape[0]):
            parts = [turned_ref[step, :, span] for span in spans]
            yield parts[0] if len(parts) == 1 else jnp.concatenate(parts, axis=1)


def columns_at(offset, part, width):
    site = lax.axis_index("site")
    places = (site, lax.axis_size("site") - 1 - site)
    held = [slice(offset, offset + part), slice(width + offset, width + offset + part)]
    return held, [pl.ds(pl.multiple_of(p * width + offset, LANES), part) for p in places]


def against(corner, product):
    return lax.dot_general(
        corner, product, (((1,), (1,)), ((), ())), preferred_element_type=jnp.float32
    )


def sum_kernel(offset, ours, theirs, *refs):
    *turned_refs, vertex_ref, out_ref = refs
    width = ours.shape[1]
    total = None
    for met_ref, held, spot in zip((ours, theirs), *columns_at(offset, ours.shape[2], width)):
        pairs = None
        for step, own in enumerate(own_levels(turned_refs, [held])):
            product = multiply(met_ref[step], own)
            pairs = product if pairs is None else pairs + product
        for half in split_halves(pairs):
            part = against(vertex_ref[:, spot], half)
            total = part if total is None else total + part
    out_ref[...] = total


def finish_kernel(offset, *refs):
    ours, theirs, hop_ref, scale_ref, vertex_ref, total_ref, *turned_refs = refs[:-3]
    out_ref, result, sems = refs[-3:]
    wraps, (sites, width) = scale_ref.shape[0], total_ref.shape
    spans = [slice(0, width), slice(width, 2 * width)]
    held, spots = columns_at(offset, ours.shape[1], width)
    other = jnp.concatenate([theirs[span, :] for span in reversed(spans)], axis=0)
    level = spread(jnp.concatenate([ours[...], other], axis=1), PIECES)
    narrow = [block.astype(jnp.bfloat16) for block in level]
    pairs = None
    for step, own in enumerate(own_levels(turned_refs, held)):
        halves = 2 if step < wraps - 1 else 1
        met, *_ = advance(step, halves, hop_ref, scale_ref, level, narrow)
        product = multiply(met, own)
        pairs = product if pairs is None else pairs + product
    halves = split_halves(pairs)
    edges = [0, sites - sites // 4, sites]
    copies = []
    for block, (begin, end) in enumerate(zip(edges, edges[1:])):
        span = slice(begin, end)
        corner = jnp.concatenate([vertex_ref[span, spot] for spot in spots], axis=1)
        total = total_ref[span, :]
        for half in halves:
            total = total + against(corner, half)
        result[span, :] = (total / wraps).astype(result.dtype)
        copy = pltpu.make_async_copy(
            result.at[pl.ds(begin, end - begin)],
            out_ref.at[pl.ds(begin, end - begin)],
            sems.at[block],
        )
        copy.start()
        copies.append(copy)
    for copy in copies:
        copy.wait()


def cut(seed, spins, spans):
    wraps, sites = spins.shape[0], seed.shape[0]
    outs = [jax.ShapeDtypeStruct((sites, b - a), jnp.bfloat16) for a, b in spans]
    outs.append(jax.ShapeDtypeStruct((wraps, sites), jnp.bfloat16))
    *pieces, lines = pl.pallas_call(
        functools.partial(cut_kernel, spans),
        out_shape=outs,
        in_specs=[HBM, HBM],
        out_specs=[VMEM] * len(outs),
        scratch_shapes=[
            pltpu.VMEM(spins.shape, spins.dtype),
            pltpu.SemaphoreType.DMA((2 * len(spans),)),
            pltpu.SemaphoreType.DMA,
        ],
        compiler_params=limit(8),
        name="cut",
    )(in_hbm(seed), in_hbm(spins))
    return pieces, lines


def hold(lines):
    return pl.pallas_call(
        hold_kernel,
        out_shape=jax.ShapeDtypeStruct(lines.shape, lines.dtype),
        in_specs=[VMEM],
        out_specs=VMEM,
        compiler_params=limit(4),
        cost_estimate=pl.CostEstimate(flops=1 << 32, bytes_accessed=1 << 24, transcendentals=0),
        name="hold",
    )(lines)


def prepare(hop_matrix, pieces):
    sites = hop_matrix.shape[0]
    width = sum(piece.shape[1] for piece in pieces)
    square = jax.ShapeDtypeStruct((sites, sites), jnp.bfloat16)
    return pl.pallas_call(
        prepare_kernel,
        out_shape=[square] * 3 + [jax.ShapeDtypeStruct((width, sites), jnp.bfloat16)],
        in_specs=[VMEM] * (1 + len(pieces)),
        out_specs=[VMEM] * 4,
        compiler_params=limit(8),
        cost_estimate=pl.CostEstimate(flops=1 << 28, bytes_accessed=1 << 22, transcendentals=0),
        name="prepare",
    )(hop_matrix, *pieces)


def lift(seed_t, high_t, low_t, vertex):
    width, sites = seed_t.shape
    return pl.pallas_call(
        lift_kernel,
        out_shape=jax.ShapeDtypeStruct((width, sites), jnp.float32),
        in_specs=[VMEM] * 4,
        out_specs=VMEM,
        compiler_params=limit(16),
        cost_estimate=work(width, sites, 2),
        name="lift",
    )(seed_t, high_t, low_t, vertex)


def join(held, came):
    shape = (held.shape[0] + came.shape[0], held.shape[1])
    return pl.pallas_call(
        join_kernel,
        out_shape=jax.ShapeDtypeStruct(shape, held.dtype),
        in_specs=[VMEM] * 2,
        out_specs=VMEM,
        compiler_params=limit(4),
        name="join",
    )(held, came)


def start_own(wraps, image, high_t, low_t, lines, doubled):
    width, sites = image.shape
    return pl.pallas_call(
        functools.partial(early_kernel, lax.axis_size("rowt"), doubled),
        out_shape=[
            jax.ShapeDtypeStruct((1, width, sites), jnp.bfloat16),
            jax.ShapeDtypeStruct((width, sites), jnp.float32),
            jax.ShapeDtypeStruct((wraps, sites), jnp.float32),
            jax.ShapeDtypeStruct((wraps, sites, LANES), jnp.float32),
        ],
        in_specs=[VMEM] * (3 + len(lines)),
        out_specs=[VMEM] * 4,
        compiler_params=limit(16),
        cost_estimate=work(width, sites, 2),
        name="early",
    )(image, high_t, low_t, *lines)


def propagate(first, last, image, high_t, low_t, scale):
    width, sites = image.shape
    wraps, steps = scale.shape[0], last - first
    outs = [jax.ShapeDtypeStruct((steps, width, sites), jnp.bfloat16)]
    if last < wraps:
        outs.append(jax.ShapeDtypeStruct((width, sites), jnp.float32))
    return pl.pallas_call(
        functools.partial(own_kernel, first),
        out_shape=outs,
        in_specs=[VMEM] * 4,
        out_specs=[VMEM] * len(outs),
        compiler_params=limit(16),
        cost_estimate=work(width, sites, 2 * steps),
    )(image, high_t, low_t, scale)


def work(columns, sites, wraps):
    return pl.CostEstimate(
        flops=wraps * sites * sites * columns // 16, bytes_accessed=1 << 16, transcendentals=0
    )


def chain(arrived, hop, scale, width):
    sites, columns = arrived.shape
    wraps = scale.shape[0]
    shape = jax.ShapeDtypeStruct((wraps, width, columns), jnp.bfloat16)
    return pl.pallas_call(
        chain_kernel,
        out_shape=[shape] * 2,
        in_specs=[VMEM] * 3,
        out_specs=[VMEM] * 2,
        compiler_params=limit(16),
        cost_estimate=work(columns, sites, wraps),
        name="chain",
    )(arrived, hop, scale)


def add_up(offset, ours, theirs, turned, vertex):
    _, width, columns = ours.shape
    sites = vertex.shape[0]
    return pl.pallas_call(
        functools.partial(sum_kernel, offset),
        out_shape=jax.ShapeDtypeStruct((sites, width), jnp.float32),
        in_specs=[VMEM] * (3 + len(turned)),
        out_specs=VMEM,
        compiler_params=limit(16),
        cost_estimate=work(columns, sites, 2),
        name="add_up",
    )(ours, theirs, *turned, vertex)


def finish(offset, ours, theirs, hop, columns, vertex, total, turned):
    sites, width = total.shape
    blocks = 2
    return pl.pallas_call(
        functools.partial(finish_kernel, offset),
        out_shape=jax.ShapeDtypeStruct((sites, width), jnp.bfloat16),
        in_specs=[VMEM] * (6 + len(turned)),
        out_specs=HBM,
        scratch_shapes=[
            pltpu.VMEM((sites, width), jnp.bfloat16),
            pltpu.SemaphoreType.DMA((blocks,)),
        ],
        compiler_params=limit(16),
        cost_estimate=work(2 * ours.shape[1], sites, columns.shape[0]),
        name="finish",
    )(ours, theirs, hop, columns, vertex, total, *turned)


def fetch_lines(lines):
    rows, count = lax.axis_size("rowt"), lines.shape[0]
    if rows == count and rows & (rows - 1) == 0:
        bit = 1
        while bit < rows:
            came = lax.ppermute(lines, "rowt", [(i, i ^ bit) for i in range(rows)])
            bit *= 2
            if bit < rows:
                lines = join(lines, came)
        return [lines, came], True
    found = []
    for step in range(count):
        line, shift = lines[step : step + 1], (step + 1) % rows
        if shift:
            line = lax.ppermute(line, "rowt", [((i + shift) % rows, i) for i in range(rows)])
        found.append(line)
    return found, False


def per_device(seed_green, field_spins, hop_matrix, vertex):
    cols, sites = lax.axis_size("colt"), lax.axis_size("site")
    wraps, width = field_spins.shape[0], seed_green.shape[-1]
    edge = width - LANES
    across = [(i, (i + cols // 2) % cols) for i in range(cols)]
    swap = [(i, sites - 1 - i) for i in range(sites)]

    pieces, lines = cut(seed_green[0, 0], field_spins, [(0, edge), (edge, width)])
    first = lax.ppermute(pieces[0], "colt", across)
    second = lax.ppermute(pieces[1], "colt", across)
    found, doubled = fetch_lines(hold(lines))
    hop, high_t, low_t, seed_t = prepare(hop_matrix, pieces)
    image = lift(seed_t, high_t, low_t, vertex)
    early, image, scale, columns = start_own(wraps, image, high_t, low_t, found, doubled)
    keep, send = chain(first, hop, columns, width)
    came = lax.ppermute(send, "site", swap)
    middle = wraps // 2
    inner, image = propagate(1, middle, image, high_t, low_t, scale)
    other = lax.ppermute(second, "site", swap)
    (late,) = propagate(middle, wraps, image, high_t, low_t, scale)
    turned = [early, inner, late]
    total = add_up(0, keep, came, turned, vertex)
    result = finish(edge, second, other, hop, columns, vertex, total, turned)
    return result[None, None]


def solution(mesh):
    return jax.shard_map(
        per_device,
        mesh=mesh,
        in_specs=(
            P(("groups", "rowt"), "colt", None, "site"),
            P(None, ("groups", "rowt"), None),
            P(),
            P(),
        ),
        out_specs=P(("groups", "rowt"), "colt", None, "site"),
        check_vma=False,
    )
```

```python
import functools

import jax
import jax.numpy as jnp
from jax import lax
from jax.experimental import pallas as pl
from jax.experimental.pallas import tpu as pltpu
from jax.sharding import PartitionSpec as P


coupling = 0.45
keep_share = 0.8
hop_share = 0.3
LANES = 128
PIECES = 4


VMEM = pl.BlockSpec(memory_space=pltpu.VMEM)
HBM = pl.BlockSpec(memory_space=pltpu.HBM)


def limit(mebibytes):
    return pltpu.CompilerParams(vmem_limit_bytes=mebibytes << 20)


def in_hbm(array):
    return pltpu.with_memory_space_constraint(array, pltpu.HBM)


def split_halves(value):
    high = value.astype(jnp.bfloat16)
    low = (value - high.astype(jnp.float32)).astype(jnp.bfloat16)
    return high, low


def site_spans(width):
    site = lax.axis_index("site")
    places = (site, lax.axis_size("site") - 1 - site)
    return [pl.ds(pl.multiple_of(place * width, LANES), width) for place in places]


def cut_kernel(spans, seed_ref, spins_ref, *refs):
    pieces, lines = refs[: len(spans)], refs[len(spans)]
    spins_in, piece_sems, spin_sem = refs[-3:]
    width = seed_ref.shape[1]
    sources = site_spans(width)
    copies = []
    for (a, b), piece in zip(spans, pieces):
        for half, source in enumerate(sources):
            copy = pltpu.make_async_copy(
                seed_ref.at[source, pl.ds(a, b - a)],
                piece.at[pl.ds(half * width, width)],
                piece_sems.at[len(copies)],
            )
            copy.start()
            copies.append(copy)
    spin_copy = pltpu.make_async_copy(spins_ref, spins_in, spin_sem)
    spin_copy.start()
    spin_copy.wait()
    parts = [spins_in[step] for step in range(lines.shape[0])]
    lines[...] = jnp.concatenate(parts, axis=0).astype(jnp.float32).astype(jnp.bfloat16)
    for copy in copies:
        copy.wait()


def hold_kernel(lines_ref, out_ref):
    out_ref[...] = lines_ref[...]


def prepare_kernel(hop_ref, *refs):
    pieces = refs[:-4]
    hop_out, high_t, low_t, turned_out = refs[-4:]
    width, _ = turned_out.shape
    start = 0
    for piece in pieces:
        turned_out[start : start + piece.shape[1], :] = piece[...].T
        start += piece.shape[1]
    site = lax.axis_index("site")
    places = (site, lax.axis_size("site") - 1 - site)
    for half, place in enumerate(places):
        for start in range(0, width, LANES):
            rows = pl.ds(pl.multiple_of(place * width + start, LANES), LANES)
            strip = jnp.concatenate([hop_ref[rows, span] for span in site_spans(width)], axis=1)
            high, low = split_halves(hop_share * strip)
            spot = slice(half * width + start, half * width + start + LANES)
            hop_out[spot, :] = high
            high_t[:, spot] = high.T
            low_t[:, spot] = low.T


def hop_turned(narrow, high_t, low_t):
    hopped = jnp.dot(narrow, high_t[...], preferred_element_type=jnp.float32)
    if low_t is not None:
        hopped += jnp.dot(narrow, low_t[...], preferred_element_type=jnp.float32)
    return hopped


def lift_kernel(seed_t, high_t, low_t, _, image_out):
    narrow = seed_t[...]
    hopped = hop_turned(narrow, high_t, low_t)
    image_out[...] = keep_share * narrow.astype(jnp.float32) + hopped


def join_kernel(held_ref, came_ref, out_ref):
    out_ref[...] = jnp.concatenate([held_ref[...], came_ref[...]], axis=0)


def early_kernel(row_count, doubled, image_ref, high_t, low_t, *refs):
    *line_refs, turned_out, image_out, scale_out, column_out = refs
    wraps = scale_out.shape[0]
    row_index = lax.axis_index("rowt")
    lines = jnp.concatenate([ref[...].astype(jnp.float32) for ref in line_refs], axis=0)
    places = lax.broadcasted_iota(jnp.int32, lines.shape, 0)
    half = lines.shape[1] // 2
    other = jnp.concatenate([lines[:, half:], lines[:, :half]], axis=1)
    lines = jnp.where(lax.axis_index("site") == 0, lines, other)
    scales = []
    for step in range(wraps):
        target = (row_index + step + 1) % row_count
        if doubled:
            pick = (row_index ^ target) * wraps + step
            spins = jnp.sum(jnp.where(places == pick, lines, 0.0), axis=0, keepdims=True)
        else:
            spins = lines[step : step + 1]
        sign = jnp.where(target == 0, -1.0, 1.0)
        scales.append(sign * jnp.exp(coupling * (2.0 * spins - 1.0)))
    turned = scales[0] * image_ref[...]
    narrow = turned.astype(jnp.bfloat16)
    turned_out[0] = narrow
    image_out[...] = keep_share * turned + hop_turned(narrow, high_t, low_t)
    scale = jnp.concatenate(scales, axis=0)
    scale_out[...] = scale
    columns = scale.T
    for step in range(wraps):
        column_out[step] = jnp.broadcast_to(columns[:, step : step + 1], column_out.shape[1:])


def rest_kernel(place, first, last, image_ref, high_t, low_t, scale_ref, *refs):
    wraps = scale_ref.shape[0]
    turned_out = refs[-1] if last == wraps else refs[-2]

    @pl.when(lax.axis_index("site") == place)
    def _():
        image = image_ref[...]
        for step in range(first, last):
            turned = scale_ref[step : step + 1, :] * image
            narrow = turned.astype(jnp.bfloat16)
            turned_out[step - 1] = narrow
            if step < wraps - 1:
                low = low_t if step < wraps - 2 else None
                image = keep_share * turned + hop_turned(narrow, high_t, low)
        if last < wraps:
            refs[-1][...] = image


def spread(columns, pieces):
    size = columns.shape[0] // pieces
    starts = range(0, columns.shape[0], size)
    return [columns[start : start + size].astype(jnp.float32) for start in starts]


def advance(step, halves, hop_ref, scale_ref, level, narrow):
    size, copies = level[0].shape[0], level[0].shape[1] // LANES
    source = jnp.concatenate(narrow, axis=0)
    new, fresh = [], []
    each = len(level) // 2
    for half in range(halves):
        for number in range(half * each, half * each + each):
            span = slice(number * size, (number + 1) * size)
            hopped = jnp.dot(hop_ref[span, :], source, preferred_element_type=jnp.float32)
            scale = jnp.concatenate([scale_ref[step, span, :]] * copies, axis=1)
            moved = scale * (keep_share * level[number] + hopped)
            new.append(moved)
            fresh.append(moved.astype(jnp.bfloat16))
        yield jnp.concatenate(fresh[half * each : half * each + each], axis=0)
    if halves == 2:
        level[:], narrow[:] = new, fresh


def chain_kernel(arrived, hop_ref, scale_ref, keep_out, send_out):
    level = spread(arrived[...], PIECES)
    narrow = [block.astype(jnp.bfloat16) for block in level]
    for step in range(keep_out.shape[0]):
        rounded = advance(step, 2, hop_ref, scale_ref, level, narrow)
        for value, out in zip(rounded, (keep_out, send_out)):
            out[step] = value


def multiply(met, own):
    return (met * own).astype(jnp.float32)


def own_levels(turned_refs, spans):
    for turned_ref in turned_refs:
        for step in range(turned_ref.shape[0]):
            parts = [turned_ref[step, :, span] for span in spans]
            yield parts[0] if len(parts) == 1 else jnp.concatenate(parts, axis=1)


def columns_at(offset, part, width):
    site = lax.axis_index("site")
    places = (site, lax.axis_size("site") - 1 - site)
    held = [slice(offset, offset + part), slice(width + offset, width + offset + part)]
    return held, [pl.ds(pl.multiple_of(p * width + offset, LANES), part) for p in places]


def against(corner, product):
    return lax.dot_general(
        corner, product, (((1,), (1,)), ((), ())), preferred_element_type=jnp.float32
    )


def sum_part(offset, which, met_ref, vertex_ref, turned_refs):
    _, width, part = met_ref.shape
    held, spots = columns_at(offset, part, width)
    pairs = None
    for step, own in enumerate(own_levels(turned_refs, [held[which]])):
        product = multiply(met_ref[step], own)
        pairs = product if pairs is None else pairs + product
    corner = vertex_ref[:, spots[which]]
    high, low = split_halves(pairs)
    return against(corner, high) + against(corner, low)


def ours_kernel(offset, place, met_ref, vertex_ref, early_ref, rest_ref, *refs):
    @pl.when(lax.axis_index("site") == place)
    def _():
        refs[-1][...] = sum_part(offset, 0, met_ref, vertex_ref, (early_ref, rest_ref))


def theirs_kernel(offset, met_ref, vertex_ref, early_ref, rest_ref, total_ref, out_ref):
    part = sum_part(offset, 1, met_ref, vertex_ref, (early_ref, rest_ref))
    out_ref[...] = total_ref[...] + part


def finish_kernel(offset, *refs):
    ours, theirs, hop_ref, scale_ref, vertex_ref, total_ref, *turned_refs = refs[:-3]
    out_ref, result, sems = refs[-3:]
    wraps, (sites, width) = scale_ref.shape[0], total_ref.shape
    spans = [slice(0, width), slice(width, 2 * width)]
    held, spots = columns_at(offset, ours.shape[1], width)
    other = jnp.concatenate([theirs[span, :] for span in reversed(spans)], axis=0)
    level = spread(jnp.concatenate([ours[...], other], axis=1), PIECES)
    narrow = [block.astype(jnp.bfloat16) for block in level]
    pairs = None
    for step, own in enumerate(own_levels(turned_refs, held)):
        halves = 2 if step < wraps - 1 else 1
        met, *_ = advance(step, halves, hop_ref, scale_ref, level, narrow)
        product = multiply(met, own)
        pairs = product if pairs is None else pairs + product
    halves = split_halves(pairs)
    edges = [0, sites - sites // 4, sites]
    copies = []
    for block, (begin, end) in enumerate(zip(edges, edges[1:])):
        span = slice(begin, end)
        corner = jnp.concatenate([vertex_ref[span, spot] for spot in spots], axis=1)
        total = total_ref[span, :]
        for half in halves:
            total = total + against(corner, half)
        result[span, :] = (total / wraps).astype(result.dtype)
        copy = pltpu.make_async_copy(
            result.at[pl.ds(begin, end - begin)],
            out_ref.at[pl.ds(begin, end - begin)],
            sems.at[block],
        )
        copy.start()
        copies.append(copy)
    for copy in copies:
        copy.wait()


def cut(seed, spins, spans):
    wraps, sites = spins.shape[0], seed.shape[0]
    outs = [jax.ShapeDtypeStruct((sites, b - a), jnp.bfloat16) for a, b in spans]
    outs.append(jax.ShapeDtypeStruct((wraps, sites), jnp.bfloat16))
    *pieces, lines = pl.pallas_call(
        functools.partial(cut_kernel, spans),
        out_shape=outs,
        in_specs=[HBM, HBM],
        out_specs=[VMEM] * len(outs),
        scratch_shapes=[
            pltpu.VMEM(spins.shape, spins.dtype),
            pltpu.SemaphoreType.DMA((2 * len(spans),)),
            pltpu.SemaphoreType.DMA,
        ],
        compiler_params=limit(8),
        name="cut",
    )(in_hbm(seed), in_hbm(spins))
    return pieces, lines


def hold(lines):
    return pl.pallas_call(
        hold_kernel,
        out_shape=jax.ShapeDtypeStruct(lines.shape, lines.dtype),
        in_specs=[VMEM],
        out_specs=VMEM,
        compiler_params=limit(4),
        cost_estimate=pl.CostEstimate(flops=1 << 32, bytes_accessed=1 << 24, transcendentals=0),
        name="hold",
    )(lines)


def prepare(hop_matrix, pieces):
    sites = hop_matrix.shape[0]
    width = sum(piece.shape[1] for piece in pieces)
    square = jax.ShapeDtypeStruct((sites, sites), jnp.bfloat16)
    return pl.pallas_call(
        prepare_kernel,
        out_shape=[square] * 3 + [jax.ShapeDtypeStruct((width, sites), jnp.bfloat16)],
        in_specs=[VMEM] * (1 + len(pieces)),
        out_specs=[VMEM] * 4,
        compiler_params=limit(8),
        cost_estimate=pl.CostEstimate(flops=1 << 28, bytes_accessed=1 << 22, transcendentals=0),
        name="prepare",
    )(hop_matrix, *pieces)


def lift(seed_t, high_t, low_t, vertex):
    width, sites = seed_t.shape
    return pl.pallas_call(
        lift_kernel,
        out_shape=jax.ShapeDtypeStruct((width, sites), jnp.float32),
        in_specs=[VMEM] * 4,
        out_specs=VMEM,
        compiler_params=limit(16),
        cost_estimate=work(width, sites, 2),
        name="lift",
    )(seed_t, high_t, low_t, vertex)


def join(held, came):
    shape = (held.shape[0] + came.shape[0], held.shape[1])
    return pl.pallas_call(
        join_kernel,
        out_shape=jax.ShapeDtypeStruct(shape, held.dtype),
        in_specs=[VMEM] * 2,
        out_specs=VMEM,
        compiler_params=limit(4),
        name="join",
    )(held, came)


def start_own(wraps, image, high_t, low_t, lines, doubled):
    width, sites = image.shape
    return pl.pallas_call(
        functools.partial(early_kernel, lax.axis_size("rowt"), doubled),
        out_shape=[
            jax.ShapeDtypeStruct((1, width, sites), jnp.bfloat16),
            jax.ShapeDtypeStruct((width, sites), jnp.float32),
            jax.ShapeDtypeStruct((wraps, sites), jnp.float32),
            jax.ShapeDtypeStruct((wraps, sites, LANES), jnp.float32),
        ],
        in_specs=[VMEM] * (3 + len(lines)),
        out_specs=[VMEM] * 4,
        compiler_params=limit(16),
        cost_estimate=work(width, sites, 2),
        name="early",
    )(image, high_t, low_t, *lines)


def propagate(place, first, last, image, high_t, low_t, scale, turned=None):
    (width, sites), wraps = image.shape, scale.shape[0]
    extra = [] if turned is None else [turned]
    outs = [jax.ShapeDtypeStruct((wraps - 1, width, sites), jnp.bfloat16)]
    if last < wraps:
        outs.append(jax.ShapeDtypeStruct((width, sites), jnp.float32))
    return pl.pallas_call(
        functools.partial(rest_kernel, place, first, last),
        out_shape=outs,
        in_specs=[VMEM] * (4 + len(extra)),
        out_specs=[VMEM] * len(outs),
        input_output_aliases={4: 0} if extra else {},
        compiler_params=limit(16),
        cost_estimate=work(width, sites, 2 * (last - first)),
    )(image, high_t, low_t, scale, *extra)


def work(columns, sites, wraps):
    return pl.CostEstimate(
        flops=wraps * sites * sites * columns // 16, bytes_accessed=1 << 16, transcendentals=0
    )


def chain(arrived, hop, scale, width):
    sites, columns = arrived.shape
    wraps = scale.shape[0]
    shape = jax.ShapeDtypeStruct((wraps, width, columns), jnp.bfloat16)
    return pl.pallas_call(
        chain_kernel,
        out_shape=[shape] * 2,
        in_specs=[VMEM] * 3,
        out_specs=[VMEM] * 2,
        compiler_params=limit(16),
        cost_estimate=work(columns, sites, wraps),
        name="chain",
    )(arrived, hop, scale)


def add_up(kernel, met, vertex, turned, total):
    _, width, columns = met.shape
    sites = vertex.shape[0]
    extra = [] if total is None else [total]
    return pl.pallas_call(
        kernel,
        out_shape=jax.ShapeDtypeStruct((sites, width), jnp.float32),
        in_specs=[VMEM] * (2 + len(turned) + len(extra)),
        out_specs=VMEM,
        input_output_aliases={2 + len(turned): 0} if extra else {},
        compiler_params=limit(16),
        cost_estimate=work(columns, sites, 1),
    )(met, vertex, *turned, *extra)


def finish(offset, ours, theirs, hop, columns, vertex, total, turned):
    sites, width = total.shape
    blocks = 2
    return pl.pallas_call(
        functools.partial(finish_kernel, offset),
        out_shape=jax.ShapeDtypeStruct((sites, width), jnp.bfloat16),
        in_specs=[VMEM] * (6 + len(turned)),
        out_specs=HBM,
        scratch_shapes=[
            pltpu.VMEM((sites, width), jnp.bfloat16),
            pltpu.SemaphoreType.DMA((blocks,)),
        ],
        compiler_params=limit(16),
        cost_estimate=work(2 * ours.shape[1], sites, columns.shape[0]),
        name="finish",
    )(ours, theirs, hop, columns, vertex, total, *turned)


def fetch_lines(lines):
    rows, count = lax.axis_size("rowt"), lines.shape[0]
    sites = lax.axis_size("site")
    if rows == count and rows & (rows - 1) == 0:
        bit = 1
        while bit < rows:
            pairs = [
                (i * sites + core, (i ^ bit) * sites + sites - 1 - core)
                for i in range(rows)
                for core in range(sites)
            ]
            came = lax.ppermute(lines, ("rowt", "site"), pairs)
            bit *= 2
            if bit < rows:
                lines = join(lines, came)
        return [lines, came], True
    found = []
    for step in range(count):
        line, shift = lines[step : step + 1], (step + 1) % rows
        if shift:
            line = lax.ppermute(line, "rowt", [((i + shift) % rows, i) for i in range(rows)])
        found.append(line)
    return found, False


def per_device(seed_green, field_spins, hop_matrix, vertex):
    cols, sites = lax.axis_size("colt"), lax.axis_size("site")
    wraps, width = field_spins.shape[0], seed_green.shape[-1]
    edge = width - LANES
    across = [(i, (i + cols // 2) % cols) for i in range(cols)]
    swap = [(i, sites - 1 - i) for i in range(sites)]

    pieces, lines = cut(seed_green[0, 0], field_spins, [(0, edge), (edge, width)])
    first = lax.ppermute(pieces[0], "colt", across)
    second = lax.ppermute(pieces[1], "colt", across)
    found, doubled = fetch_lines(hold(lines))
    hop, high_t, low_t, seed_t = prepare(hop_matrix, pieces)
    image = lift(seed_t, high_t, low_t, vertex)
    early, image, scale, columns = start_own(wraps, image, high_t, low_t, found, doubled)
    own = (high_t, low_t, scale)
    rest, level = propagate(0, 1, 2, image, *own)
    keep, send = chain(first, hop, columns, width)
    for place in range(1, sites):
        (rest,) = propagate(place, 1, wraps, image, *own, rest)
    came = lax.ppermute(send, "site", swap)
    (rest,) = propagate(0, 2, wraps, level, *own, rest)
    turned = [early, rest]
    total = None
    for place in range(1, sites):
        kernel = functools.partial(ours_kernel, 0, place)
        total = add_up(kernel, keep, vertex, turned, total)
    other = lax.ppermute(second, "site", swap)
    total = add_up(functools.partial(ours_kernel, 0, 0), keep, vertex, turned, total)
    total = add_up(functools.partial(theirs_kernel, 0), came, vertex, turned, total)
    result = finish(edge, second, other, hop, columns, vertex, total, turned)
    return result[None, None]


def solution(mesh):
    return jax.shard_map(
        per_device,
        mesh=mesh,
        in_specs=(
            P(("groups", "rowt"), "colt", None, "site"),
            P(None, ("groups", "rowt"), None),
            P(),
            P(),
        ),
        out_specs=P(("groups", "rowt"), "colt", None, "site"),
        check_vma=False,
    )
```

```python
import functools

import jax
import jax.numpy as jnp
from jax import lax
from jax.experimental import pallas as pl
from jax.experimental.pallas import tpu as pltpu
from jax.sharding import PartitionSpec as P


coupling = 0.45
keep_share = 0.8
hop_share = 0.3
LANES = 128
PIECES = 4


VMEM = pl.BlockSpec(memory_space=pltpu.VMEM)
HBM = pl.BlockSpec(memory_space=pltpu.HBM)


def limit(mebibytes):
    return pltpu.CompilerParams(vmem_limit_bytes=mebibytes << 20)


def in_hbm(array):
    return pltpu.with_memory_space_constraint(array, pltpu.HBM)


def split_halves(value):
    high = value.astype(jnp.bfloat16)
    low = (value - high.astype(jnp.float32)).astype(jnp.bfloat16)
    return high, low


def site_spans(width):
    site = lax.axis_index("site")
    places = (site, lax.axis_size("site") - 1 - site)
    return [pl.ds(pl.multiple_of(place * width, LANES), width) for place in places]


def cut_kernel(spans, seed_ref, spins_ref, *refs):
    pieces, lines = refs[: len(spans)], refs[len(spans)]
    spins_in, piece_sems, spin_sem = refs[-3:]
    width = seed_ref.shape[1]
    sources = site_spans(width)
    copies = []
    for (a, b), piece in zip(spans, pieces):
        for half, source in enumerate(reversed(sources)):
            copy = pltpu.make_async_copy(
                seed_ref.at[source, pl.ds(a, b - a)],
                piece.at[pl.ds(half * width, width)],
                piece_sems.at[len(copies)],
            )
            copy.start()
            copies.append(copy)
    spin_copy = pltpu.make_async_copy(spins_ref, spins_in, spin_sem)
    spin_copy.start()
    spin_copy.wait()
    parts = [spins_in[step] for step in range(lines.shape[0])]
    lines[...] = jnp.concatenate(parts, axis=0).astype(jnp.float32).astype(jnp.bfloat16)
    for copy in copies:
        copy.wait()


def hold_kernel(lines_ref, out_ref):
    out_ref[...] = lines_ref[...]


def prepare_kernel(hop_ref, *refs):
    pieces = refs[:-4]
    hop_out, high_t, low_t, turned_out = refs[-4:]
    width, _ = turned_out.shape
    start = 0
    for piece in pieces:
        lines = slice(start, start + piece.shape[1])
        turned_out[lines, :width] = piece[width:, :].T
        turned_out[lines, width:] = piece[:width, :].T
        start += piece.shape[1]
    site = lax.axis_index("site")
    places = (site, lax.axis_size("site") - 1 - site)
    for half, place in enumerate(places):
        for start in range(0, width, LANES):
            rows = pl.ds(pl.multiple_of(place * width + start, LANES), LANES)
            strip = jnp.concatenate([hop_ref[rows, span] for span in site_spans(width)], axis=1)
            high, low = split_halves(hop_share * strip)
            spot = slice(half * width + start, half * width + start + LANES)
            hop_out[spot, :] = high
            high_t[:, spot] = high.T
            low_t[:, spot] = low.T


def hop_turned(narrow, high_t, low_t):
    hopped = jnp.dot(narrow, high_t[...], preferred_element_type=jnp.float32)
    if low_t is not None:
        hopped += jnp.dot(narrow, low_t[...], preferred_element_type=jnp.float32)
    return hopped


def lift_kernel(seed_t, high_t, low_t, _, image_out):
    narrow = seed_t[...]
    hopped = hop_turned(narrow, high_t, low_t)
    image_out[...] = keep_share * narrow.astype(jnp.float32) + hopped


def join_kernel(held_ref, came_ref, out_ref):
    out_ref[...] = jnp.concatenate([held_ref[...], came_ref[...]], axis=0)


def early_kernel(row_count, doubled, image_ref, high_t, low_t, *refs):
    *line_refs, turned_out, image_out, scale_out, column_out = refs
    wraps = scale_out.shape[0]
    row_index = lax.axis_index("rowt")
    lines = jnp.concatenate([ref[...].astype(jnp.float32) for ref in line_refs], axis=0)
    places = lax.broadcasted_iota(jnp.int32, lines.shape, 0)
    half = lines.shape[1] // 2
    other = jnp.concatenate([lines[:, half:], lines[:, :half]], axis=1)
    lines = jnp.where(lax.axis_index("site") == 0, lines, other)
    scales = []
    for step in range(wraps):
        target = (row_index + step + 1) % row_count
        if doubled:
            pick = (row_index ^ target) * wraps + step
            spins = jnp.sum(jnp.where(places == pick, lines, 0.0), axis=0, keepdims=True)
        else:
            spins = lines[step : step + 1]
        sign = jnp.where(target == 0, -1.0, 1.0)
        scales.append(sign * jnp.exp(coupling * (2.0 * spins - 1.0)))
    turned = scales[0] * image_ref[...]
    narrow = turned.astype(jnp.bfloat16)
    turned_out[0] = narrow
    image_out[...] = keep_share * turned + hop_turned(narrow, high_t, low_t)
    scale = jnp.concatenate(scales, axis=0)
    scale_out[...] = scale
    columns = scale.T
    for step in range(wraps):
        column_out[step] = jnp.broadcast_to(columns[:, step : step + 1], column_out.shape[1:])


def own_kernel(first, image_ref, high_t, low_t, scale_ref, turned_out, *rest):
    steps, wraps = turned_out.shape[0], scale_ref.shape[0]
    image = image_ref[...]
    for step in range(first, first + steps):
        turned = scale_ref[step : step + 1, :] * image
        narrow = turned.astype(jnp.bfloat16)
        turned_out[step - first] = narrow
        if step < wraps - 1:
            low = low_t if step < wraps - 2 else None
            image = keep_share * turned + hop_turned(narrow, high_t, low)
    if rest:
        rest[0][...] = image


def spread(columns, pieces):
    size = columns.shape[0] // pieces
    starts = range(0, columns.shape[0], size)
    return [columns[start : start + size].astype(jnp.float32) for start in starts]


def advance(step, halves, hop_ref, scale_ref, level, narrow):
    size, copies = level[0].shape[0], level[0].shape[1] // LANES
    source = jnp.concatenate(narrow, axis=0)
    new, fresh = [], []
    each = len(level) // 2
    for half in range(halves):
        for number in range(half * each, half * each + each):
            span = slice(number * size, (number + 1) * size)
            hopped = jnp.dot(hop_ref[span, :], source, preferred_element_type=jnp.float32)
            scale = jnp.concatenate([scale_ref[step, span, :]] * copies, axis=1)
            moved = scale * (keep_share * level[number] + hopped)
            new.append(moved)
            fresh.append(moved.astype(jnp.bfloat16))
        yield jnp.concatenate(fresh[half * each : half * each + each], axis=0)
    if halves == 2:
        level[:], narrow[:] = new, fresh


def chain_kernel(arrived, hop_ref, scale_ref, keep_out, send_out):
    level = spread(arrived[...], PIECES)
    narrow = [block.astype(jnp.bfloat16) for block in level]
    for step in range(keep_out.shape[0]):
        rounded = advance(step, 2, hop_ref, scale_ref, level, narrow)
        for value, out in zip(rounded, (keep_out, send_out)):
            out[step] = value


def multiply(met, own):
    return (met * own).astype(jnp.float32)


def own_levels(turned_refs, spans):
    for turned_ref in turned_refs:
        for step in range(turned_ref.shape[0]):
            parts = [turned_ref[step, :, span] for span in spans]
            yield parts[0] if len(parts) == 1 else jnp.concatenate(parts, axis=1)


def columns_at(offset, part, width):
    site = lax.axis_index("site")
    places = (lax.axis_size("site") - 1 - site, site)
    held = [slice(width + offset, width + offset + part), slice(offset, offset + part)]
    return held, [pl.ds(pl.multiple_of(p * width + offset, LANES), part) for p in places]


def against(corner, product):
    return lax.dot_general(
        corner, product, (((1,), (1,)), ((), ())), preferred_element_type=jnp.float32
    )


def sum_part(offset, which, met_ref, vertex_ref, turned_refs):
    _, width, part = met_ref.shape
    held, spots = columns_at(offset, part, width)
    pairs = None
    for step, own in enumerate(own_levels(turned_refs, [held[which]])):
        product = multiply(met_ref[step], own)
        pairs = product if pairs is None else pairs + product
    corner = vertex_ref[:, spots[which]]
    high, low = split_halves(pairs)
    return against(corner, high) + against(corner, low)


def add_kernel(offset, which, met_ref, vertex_ref, *refs):
    *turned_refs, out_ref = refs
    total = turned_refs.pop(0)[...] if which else 0.0
    out_ref[...] = total + sum_part(offset, which, met_ref, vertex_ref, turned_refs)


def finish_kernel(offset, *refs):
    ours, theirs, hop_ref, scale_ref, vertex_ref, total_ref, *turned_refs = refs[:-3]
    out_ref, result, sems = refs[-3:]
    wraps, (sites, width) = scale_ref.shape[0], total_ref.shape
    spans = [slice(0, width), slice(width, 2 * width)]
    held, spots = columns_at(offset, ours.shape[1], width)
    other = jnp.concatenate([theirs[span, :] for span in reversed(spans)], axis=0)
    level = spread(jnp.concatenate([ours[...], other], axis=1), PIECES)
    narrow = [block.astype(jnp.bfloat16) for block in level]
    pairs = None
    for step, own in enumerate(own_levels(turned_refs, held)):
        halves = 2 if step < wraps - 1 else 1
        met, *_ = advance(step, halves, hop_ref, scale_ref, level, narrow)
        product = multiply(met, own)
        pairs = product if pairs is None else pairs + product
    summed = pairs.astype(jnp.bfloat16)
    edges = [0, sites - sites // 4, sites]
    copies = []
    for block, (begin, end) in enumerate(zip(edges, edges[1:])):
        span = slice(begin, end)
        corner = jnp.concatenate([vertex_ref[span, spot] for spot in spots], axis=1)
        total = total_ref[span, :] + against(corner, summed)
        result[span, :] = (total / wraps).astype(result.dtype)
        copy = pltpu.make_async_copy(
            result.at[pl.ds(begin, end - begin)],
            out_ref.at[pl.ds(begin, end - begin)],
            sems.at[block],
        )
        copy.start()
        copies.append(copy)
    for copy in copies:
        copy.wait()


def cut(seed, spins, spans):
    wraps, sites = spins.shape[0], seed.shape[0]
    outs = [jax.ShapeDtypeStruct((sites, b - a), jnp.bfloat16) for a, b in spans]
    outs.append(jax.ShapeDtypeStruct((wraps, sites), jnp.bfloat16))
    *pieces, lines = pl.pallas_call(
        functools.partial(cut_kernel, spans),
        out_shape=outs,
        in_specs=[HBM, HBM],
        out_specs=[VMEM] * len(outs),
        scratch_shapes=[
            pltpu.VMEM(spins.shape, spins.dtype),
            pltpu.SemaphoreType.DMA((2 * len(spans),)),
            pltpu.SemaphoreType.DMA,
        ],
        compiler_params=limit(8),
        name="cut",
    )(in_hbm(seed), in_hbm(spins))
    return pieces, lines


def hold(lines):
    return pl.pallas_call(
        hold_kernel,
        out_shape=jax.ShapeDtypeStruct(lines.shape, lines.dtype),
        in_specs=[VMEM],
        out_specs=VMEM,
        compiler_params=limit(4),
        cost_estimate=pl.CostEstimate(flops=1 << 32, bytes_accessed=1 << 24, transcendentals=0),
        name="hold",
    )(lines)


def prepare(hop_matrix, pieces):
    sites = hop_matrix.shape[0]
    width = sum(piece.shape[1] for piece in pieces)
    square = jax.ShapeDtypeStruct((sites, sites), jnp.bfloat16)
    return pl.pallas_call(
        prepare_kernel,
        out_shape=[square] * 3 + [jax.ShapeDtypeStruct((width, sites), jnp.bfloat16)],
        in_specs=[VMEM] * (1 + len(pieces)),
        out_specs=[VMEM] * 4,
        compiler_params=limit(8),
        cost_estimate=pl.CostEstimate(flops=1 << 28, bytes_accessed=1 << 22, transcendentals=0),
        name="prepare",
    )(hop_matrix, *pieces)


def lift(seed_t, high_t, low_t, vertex):
    width, sites = seed_t.shape
    return pl.pallas_call(
        lift_kernel,
        out_shape=jax.ShapeDtypeStruct((width, sites), jnp.float32),
        in_specs=[VMEM] * 4,
        out_specs=VMEM,
        compiler_params=limit(16),
        cost_estimate=work(width, sites, 2),
        name="lift",
    )(seed_t, high_t, low_t, vertex)


def join(held, came):
    shape = (held.shape[0] + came.shape[0], held.shape[1])
    return pl.pallas_call(
        join_kernel,
        out_shape=jax.ShapeDtypeStruct(shape, held.dtype),
        in_specs=[VMEM] * 2,
        out_specs=VMEM,
        compiler_params=limit(4),
        name="join",
    )(held, came)


def start_own(wraps, image, high_t, low_t, lines, doubled):
    width, sites = image.shape
    return pl.pallas_call(
        functools.partial(early_kernel, lax.axis_size("rowt"), doubled),
        out_shape=[
            jax.ShapeDtypeStruct((1, width, sites), jnp.bfloat16),
            jax.ShapeDtypeStruct((width, sites), jnp.float32),
            jax.ShapeDtypeStruct((wraps, sites), jnp.float32),
            jax.ShapeDtypeStruct((wraps, sites, LANES), jnp.float32),
        ],
        in_specs=[VMEM] * (3 + len(lines)),
        out_specs=[VMEM] * 4,
        compiler_params=limit(16),
        cost_estimate=work(width, sites, 2),
        name="early",
    )(image, high_t, low_t, *lines)


def propagate(first, last, image, high_t, low_t, scale):
    (width, sites), wraps = image.shape, scale.shape[0]
    outs = [jax.ShapeDtypeStruct((last - first, width, sites), jnp.bfloat16)]
    if last < wraps:
        outs.append(jax.ShapeDtypeStruct((width, sites), jnp.float32))
    return pl.pallas_call(
        functools.partial(own_kernel, first),
        out_shape=outs,
        in_specs=[VMEM] * 4,
        out_specs=[VMEM] * len(outs),
        compiler_params=limit(16),
        cost_estimate=work(width, sites, 2 * (last - first)),
    )(image, high_t, low_t, scale)


def work(columns, sites, wraps):
    return pl.CostEstimate(
        flops=wraps * sites * sites * columns // 16, bytes_accessed=1 << 16, transcendentals=0
    )


def chain(arrived, hop, scale, width):
    sites, columns = arrived.shape
    wraps = scale.shape[0]
    shape = jax.ShapeDtypeStruct((wraps, width, columns), jnp.bfloat16)
    return pl.pallas_call(
        chain_kernel,
        out_shape=[shape] * 2,
        in_specs=[VMEM] * 3,
        out_specs=[VMEM] * 2,
        compiler_params=limit(16),
        cost_estimate=work(columns, sites, wraps),
        name="chain",
    )(arrived, hop, scale)


def add_up(offset, met, vertex, turned, total=None):
    _, width, columns = met.shape
    sites = vertex.shape[0]
    extra = [] if total is None else [total]
    return pl.pallas_call(
        functools.partial(add_kernel, offset, len(extra)),
        out_shape=jax.ShapeDtypeStruct((sites, width), jnp.float32),
        in_specs=[VMEM] * (2 + len(extra) + len(turned)),
        out_specs=VMEM,
        compiler_params=limit(16),
        cost_estimate=work(columns, sites, 1),
    )(met, vertex, *extra, *turned)


def finish(offset, ours, theirs, hop, columns, vertex, total, turned):
    sites, width = total.shape
    blocks = 2
    return pl.pallas_call(
        functools.partial(finish_kernel, offset),
        out_shape=jax.ShapeDtypeStruct((sites, width), jnp.bfloat16),
        in_specs=[VMEM] * (6 + len(turned)),
        out_specs=HBM,
        scratch_shapes=[
            pltpu.VMEM((sites, width), jnp.bfloat16),
            pltpu.SemaphoreType.DMA((blocks,)),
        ],
        compiler_params=limit(16),
        cost_estimate=work(2 * ours.shape[1], sites, columns.shape[0]),
        name="finish",
    )(ours, theirs, hop, columns, vertex, total, *turned)


def fetch_lines(lines):
    rows, count = lax.axis_size("rowt"), lines.shape[0]
    sites = lax.axis_size("site")
    if rows == count and rows & (rows - 1) == 0:
        bit = 1
        while bit < rows:
            pairs = [
                (i * sites + core, (i ^ bit) * sites + sites - 1 - core)
                for i in range(rows)
                for core in range(sites)
            ]
            came = lax.ppermute(lines, ("rowt", "site"), pairs)
            bit *= 2
            if bit < rows:
                lines = join(lines, came)
        return [lines, came], True
    found = []
    for step in range(count):
        line, shift = lines[step : step + 1], (step + 1) % rows
        if shift:
            line = lax.ppermute(line, "rowt", [((i + shift) % rows, i) for i in range(rows)])
        found.append(line)
    return found, False


def per_device(seed_green, field_spins, hop_matrix, vertex):
    cols, sites = lax.axis_size("colt"), lax.axis_size("site")
    wraps, width = field_spins.shape[0], seed_green.shape[-1]
    edge = width - LANES
    across = [
        (i * sites + core, (i + cols // 2) % cols * sites + sites - 1 - core)
        for i in range(cols)
        for core in range(sites)
    ]
    swap = [(i, sites - 1 - i) for i in range(sites)]

    pieces, lines = cut(seed_green[0, 0], field_spins, [(0, edge), (edge, width)])
    first = lax.ppermute(pieces[0], ("colt", "site"), across)
    second = lax.ppermute(pieces[1], ("colt", "site"), across)
    found, doubled = fetch_lines(hold(lines))
    hop, high_t, low_t, seed_t = prepare(hop_matrix, pieces)
    image = lift(seed_t, high_t, low_t, vertex)
    early, image, scale, columns = start_own(wraps, image, high_t, low_t, found, doubled)
    own = (high_t, low_t, scale)
    middle, level = propagate(1, 2, image, *own)
    keep, send = chain(first, hop, columns, width)
    came = lax.ppermute(send, "site", swap)
    (rest,) = propagate(2, wraps, level, *own)
    other = lax.ppermute(second, "site", swap)
    turned = [early, middle, rest]
    total = add_up(0, keep, vertex, turned)
    total = add_up(0, came, vertex, turned, total)
    result = finish(edge, second, other, hop, columns, vertex, total, turned)
    return result[None, None]


def solution(mesh):
    return jax.shard_map(
        per_device,
        mesh=mesh,
        in_specs=(
            P(("groups", "rowt"), "colt", None, "site"),
            P(None, ("groups", "rowt"), None),
            P(),
            P(),
        ),
        out_specs=P(("groups", "rowt"), "colt", None, "site"),
        check_vma=False,
    )
```

```python
import functools

import jax
import jax.numpy as jnp
from jax import lax
from jax.experimental import pallas as pl
from jax.experimental.pallas import tpu as pltpu
from jax.sharding import PartitionSpec as P


coupling = 0.45
keep_share = 0.8
hop_share = 0.3
LANES = 128
PIECES = 4


VMEM = pl.BlockSpec(memory_space=pltpu.VMEM)
HBM = pl.BlockSpec(memory_space=pltpu.HBM)


def limit(mebibytes):
    return pltpu.CompilerParams(vmem_limit_bytes=mebibytes << 20)


def in_hbm(array):
    return pltpu.with_memory_space_constraint(array, pltpu.HBM)


def split_halves(value):
    high = value.astype(jnp.bfloat16)
    low = (value - high.astype(jnp.float32)).astype(jnp.bfloat16)
    return high, low


def site_spans(width):
    site = lax.axis_index("site")
    places = (site, lax.axis_size("site") - 1 - site)
    return [pl.ds(pl.multiple_of(place * width, LANES), width) for place in places]


def cut_kernel(spans, seed_ref, spins_ref, *refs):
    pieces, lines = refs[: len(spans)], refs[len(spans)]
    spins_in, piece_sems, spin_sem = refs[-3:]
    width = seed_ref.shape[1]
    sources = site_spans(width)
    copies = []
    for (a, b), piece in zip(spans, pieces):
        for half, source in enumerate(reversed(sources)):
            copy = pltpu.make_async_copy(
                seed_ref.at[source, pl.ds(a, b - a)],
                piece.at[pl.ds(half * width, width)],
                piece_sems.at[len(copies)],
            )
            copy.start()
            copies.append(copy)
    spin_copy = pltpu.make_async_copy(spins_ref, spins_in, spin_sem)
    spin_copy.start()
    spin_copy.wait()
    parts = [spins_in[step] for step in range(lines.shape[0])]
    lines[...] = jnp.concatenate(parts, axis=0).astype(jnp.float32).astype(jnp.bfloat16)
    for copy in copies:
        copy.wait()


def hold_kernel(lines_ref, out_ref):
    out_ref[...] = lines_ref[...]


def prepare_kernel(hop_ref, *refs):
    pieces = refs[:-4]
    hop_out, high_t, low_t, turned_out = refs[-4:]
    width, _ = turned_out.shape
    start = 0
    for piece in pieces:
        lines = slice(start, start + piece.shape[1])
        turned_out[lines, :width] = piece[width:, :].T
        turned_out[lines, width:] = piece[:width, :].T
        start += piece.shape[1]
    site = lax.axis_index("site")
    places = (site, lax.axis_size("site") - 1 - site)
    for half, place in enumerate(places):
        for start in range(0, width, LANES):
            rows = pl.ds(pl.multiple_of(place * width + start, LANES), LANES)
            strip = jnp.concatenate([hop_ref[rows, span] for span in site_spans(width)], axis=1)
            high, low = split_halves(hop_share * strip)
            spot = slice(half * width + start, half * width + start + LANES)
            hop_out[spot, :] = high
            high_t[:, spot] = high.T
            low_t[:, spot] = low.T


def hop_turned(narrow, high_t, low_t):
    hopped = jnp.dot(narrow, high_t[...], preferred_element_type=jnp.float32)
    if low_t is not None:
        hopped += jnp.dot(narrow, low_t[...], preferred_element_type=jnp.float32)
    return hopped


def lift_kernel(seed_t, high_t, low_t, _, image_out):
    narrow = seed_t[...]
    hopped = hop_turned(narrow, high_t, low_t)
    image_out[...] = keep_share * narrow.astype(jnp.float32) + hopped


def join_kernel(held_ref, came_ref, out_ref):
    out_ref[...] = jnp.concatenate([held_ref[...], came_ref[...]], axis=0)


def early_kernel(row_count, doubled, image_ref, high_t, low_t, *refs):
    *line_refs, turned_out, image_out, scale_out, column_out = refs
    wraps = scale_out.shape[0]
    row_index = lax.axis_index("rowt")
    lines = jnp.concatenate([ref[...].astype(jnp.float32) for ref in line_refs], axis=0)
    places = lax.broadcasted_iota(jnp.int32, lines.shape, 0)
    half = lines.shape[1] // 2
    other = jnp.concatenate([lines[:, half:], lines[:, :half]], axis=1)
    lines = jnp.where(lax.axis_index("site") == 0, lines, other)
    scales = []
    for step in range(wraps):
        target = (row_index + step + 1) % row_count
        if doubled:
            pick = (row_index ^ target) * wraps + step
            spins = jnp.sum(jnp.where(places == pick, lines, 0.0), axis=0, keepdims=True)
        else:
            spins = lines[step : step + 1]
        sign = jnp.where(target == 0, -1.0, 1.0)
        scales.append(sign * jnp.exp(coupling * (2.0 * spins - 1.0)))
    turned = scales[0] * image_ref[...]
    narrow = turned.astype(jnp.bfloat16)
    turned_out[0] = narrow
    image_out[...] = keep_share * turned + hop_turned(narrow, high_t, low_t)
    scale = jnp.concatenate(scales, axis=0)
    scale_out[...] = scale
    columns = scale.T
    for step in range(wraps):
        column_out[step] = jnp.broadcast_to(columns[:, step : step + 1], column_out.shape[1:])


def own_kernel(first, image_ref, high_t, low_t, scale_ref, turned_out, *rest):
    steps, wraps = turned_out.shape[0], scale_ref.shape[0]
    image = image_ref[...]
    for step in range(first, first + steps):
        turned = scale_ref[step : step + 1, :] * image
        narrow = turned.astype(jnp.bfloat16)
        turned_out[step - first] = narrow
        if step < wraps - 1:
            low = low_t if step < wraps - 2 else None
            image = keep_share * turned + hop_turned(narrow, high_t, low)
    if rest:
        rest[0][...] = image


def spread(columns, pieces):
    size = columns.shape[0] // pieces
    starts = range(0, columns.shape[0], size)
    return [columns[start : start + size].astype(jnp.float32) for start in starts]


def advance(step, halves, hop_ref, scale_ref, level, narrow):
    size, copies = level[0].shape[0], level[0].shape[1] // LANES
    source = jnp.concatenate(narrow, axis=0)
    new, fresh = [], []
    each = len(level) // 2
    for half in range(halves):
        for number in range(half * each, half * each + each):
            span = slice(number * size, (number + 1) * size)
            hopped = jnp.dot(hop_ref[span, :], source, preferred_element_type=jnp.float32)
            scale = jnp.concatenate([scale_ref[step, span, :]] * copies, axis=1)
            moved = scale * (keep_share * level[number] + hopped)
            new.append(moved)
            fresh.append(moved.astype(jnp.bfloat16))
        yield jnp.concatenate(fresh[half * each : half * each + each], axis=0)
    level[: len(new)] = new
    if halves == 2:
        narrow[:] = fresh


def chain_kernel(arrived, hop_ref, scale_ref, keep_out, send_out):
    level = spread(arrived[...], PIECES)
    narrow = [block.astype(jnp.bfloat16) for block in level]
    for step in range(keep_out.shape[0]):
        rounded = advance(step, 2, hop_ref, scale_ref, level, narrow)
        for value, out in zip(rounded, (keep_out, send_out)):
            out[step] = value


def multiply(met, own):
    return (met * own).astype(jnp.float32)


def own_levels(turned_refs, spans):
    for turned_ref in turned_refs:
        for step in range(turned_ref.shape[0]):
            parts = [turned_ref[step, :, span] for span in spans]
            yield parts[0] if len(parts) == 1 else jnp.concatenate(parts, axis=1)


def columns_at(offset, part, width):
    site = lax.axis_index("site")
    places = (lax.axis_size("site") - 1 - site, site)
    held = [slice(width + offset, width + offset + part), slice(offset, offset + part)]
    return held, [pl.ds(pl.multiple_of(p * width + offset, LANES), part) for p in places]


def against(corner, product):
    return lax.dot_general(
        corner, product, (((1,), (1,)), ((), ())), preferred_element_type=jnp.float32
    )


def sum_part(offset, which, met_ref, vertex_ref, turned_refs):
    _, width, part = met_ref.shape
    held, spots = columns_at(offset, part, width)
    pairs = None
    for step, own in enumerate(own_levels(turned_refs, [held[which]])):
        product = multiply(met_ref[step], own)
        pairs = product if pairs is None else pairs + product
    corner = vertex_ref[:, spots[which]]
    high, low = split_halves(pairs)
    return against(corner, high) + against(corner, low)


def add_kernel(offset, which, met_ref, vertex_ref, *refs):
    *turned_refs, out_ref = refs
    total = turned_refs.pop(0)[...] if which else 0.0
    out_ref[...] = total + sum_part(offset, which, met_ref, vertex_ref, turned_refs)


def fold_kernel(hop_ref, scale_ref, fold_out):
    width, wraps = fold_out.shape[0], scale_ref.shape[0]
    left = hop_ref[:width, :].astype(jnp.float32) * scale_ref[wraps - 2 : wraps - 1, :]
    right = jnp.dot(
        left.astype(jnp.bfloat16), hop_ref[...], preferred_element_type=jnp.float32
    )
    fold_out[...] = (keep_share * left + right).astype(jnp.bfloat16)


def finish_kernel(offset, *refs):
    ours, theirs, hop_ref, fold_ref, scale_ref, vertex_ref, total_ref, *turned_refs = refs[:-3]
    out_ref, result, sems = refs[-3:]
    wraps, (sites, width) = scale_ref.shape[0], total_ref.shape
    spans = [slice(0, width), slice(width, 2 * width)]
    held, spots = columns_at(offset, ours.shape[1], width)
    other = jnp.concatenate([theirs[span, :] for span in reversed(spans)], axis=0)
    level = spread(jnp.concatenate([ours[...], other], axis=1), PIECES)
    narrow = [block.astype(jnp.bfloat16) for block in level]
    pairs = None
    for step, own in enumerate(own_levels(turned_refs, held)):
        if step < wraps - 2:
            met, *_ = advance(step, 2, hop_ref, scale_ref, level, narrow)
        else:
            weights = hop_ref if step == wraps - 2 else fold_ref
            met, *_ = advance(step, 1, weights, scale_ref, level, narrow)
        product = multiply(met, own)
        pairs = product if pairs is None else pairs + product
    summed = pairs.astype(jnp.bfloat16)
    edges = [0, sites // 2, sites]
    copies = []
    for block, (begin, end) in enumerate(zip(edges, edges[1:])):
        span = slice(begin, end)
        corner = jnp.concatenate([vertex_ref[span, spot] for spot in spots], axis=1)
        total = total_ref[span, :] + against(corner, summed)
        result[span, :] = (total / wraps).astype(result.dtype)
        copy = pltpu.make_async_copy(
            result.at[pl.ds(begin, end - begin)],
            out_ref.at[pl.ds(begin, end - begin)],
            sems.at[block],
        )
        copy.start()
        copies.append(copy)
    for copy in copies:
        copy.wait()


def cut(seed, spins, spans):
    wraps, sites = spins.shape[0], seed.shape[0]
    outs = [jax.ShapeDtypeStruct((sites, b - a), jnp.bfloat16) for a, b in spans]
    outs.append(jax.ShapeDtypeStruct((wraps, sites), jnp.bfloat16))
    *pieces, lines = pl.pallas_call(
        functools.partial(cut_kernel, spans),
        out_shape=outs,
        in_specs=[HBM, HBM],
        out_specs=[VMEM] * len(outs),
        scratch_shapes=[
            pltpu.VMEM(spins.shape, spins.dtype),
            pltpu.SemaphoreType.DMA((2 * len(spans),)),
            pltpu.SemaphoreType.DMA,
        ],
        compiler_params=limit(8),
        name="cut",
    )(in_hbm(seed), in_hbm(spins))
    return pieces, lines


def hold(lines):
    return pl.pallas_call(
        hold_kernel,
        out_shape=jax.ShapeDtypeStruct(lines.shape, lines.dtype),
        in_specs=[VMEM],
        out_specs=VMEM,
        compiler_params=limit(4),
        cost_estimate=pl.CostEstimate(flops=1 << 32, bytes_accessed=1 << 24, transcendentals=0),
        name="hold",
    )(lines)


def prepare(hop_matrix, pieces):
    sites = hop_matrix.shape[0]
    width = sum(piece.shape[1] for piece in pieces)
    square = jax.ShapeDtypeStruct((sites, sites), jnp.bfloat16)
    return pl.pallas_call(
        prepare_kernel,
        out_shape=[square] * 3 + [jax.ShapeDtypeStruct((width, sites), jnp.bfloat16)],
        in_specs=[VMEM] * (1 + len(pieces)),
        out_specs=[VMEM] * 4,
        compiler_params=limit(8),
        cost_estimate=pl.CostEstimate(flops=1 << 28, bytes_accessed=1 << 22, transcendentals=0),
        name="prepare",
    )(hop_matrix, *pieces)


def lift(seed_t, high_t, low_t, vertex):
    width, sites = seed_t.shape
    return pl.pallas_call(
        lift_kernel,
        out_shape=jax.ShapeDtypeStruct((width, sites), jnp.float32),
        in_specs=[VMEM] * 4,
        out_specs=VMEM,
        compiler_params=limit(16),
        cost_estimate=work(width, sites, 2),
        name="lift",
    )(seed_t, high_t, low_t, vertex)


def join(held, came):
    shape = (held.shape[0] + came.shape[0], held.shape[1])
    return pl.pallas_call(
        join_kernel,
        out_shape=jax.ShapeDtypeStruct(shape, held.dtype),
        in_specs=[VMEM] * 2,
        out_specs=VMEM,
        compiler_params=limit(4),
        name="join",
    )(held, came)


def start_own(wraps, image, high_t, low_t, lines, doubled):
    width, sites = image.shape
    return pl.pallas_call(
        functools.partial(early_kernel, lax.axis_size("rowt"), doubled),
        out_shape=[
            jax.ShapeDtypeStruct((1, width, sites), jnp.bfloat16),
            jax.ShapeDtypeStruct((width, sites), jnp.float32),
            jax.ShapeDtypeStruct((wraps, sites), jnp.float32),
            jax.ShapeDtypeStruct((wraps, sites, LANES), jnp.float32),
        ],
        in_specs=[VMEM] * (3 + len(lines)),
        out_specs=[VMEM] * 4,
        compiler_params=limit(16),
        cost_estimate=work(width, sites, 2),
        name="early",
    )(image, high_t, low_t, *lines)


def propagate(first, last, image, high_t, low_t, scale):
    (width, sites), wraps = image.shape, scale.shape[0]
    outs = [jax.ShapeDtypeStruct((last - first, width, sites), jnp.bfloat16)]
    if last < wraps:
        outs.append(jax.ShapeDtypeStruct((width, sites), jnp.float32))
    return pl.pallas_call(
        functools.partial(own_kernel, first),
        out_shape=outs,
        in_specs=[VMEM] * 4,
        out_specs=[VMEM] * len(outs),
        compiler_params=limit(16),
        cost_estimate=work(width, sites, 2 * (last - first)),
    )(image, high_t, low_t, scale)


def work(columns, sites, wraps):
    return pl.CostEstimate(
        flops=wraps * sites * sites * columns // 16, bytes_accessed=1 << 16, transcendentals=0
    )


def chain(arrived, hop, scale, width):
    sites, columns = arrived.shape
    wraps = scale.shape[0]
    shape = jax.ShapeDtypeStruct((wraps, width, columns), jnp.bfloat16)
    return pl.pallas_call(
        chain_kernel,
        out_shape=[shape] * 2,
        in_specs=[VMEM] * 3,
        out_specs=[VMEM] * 2,
        compiler_params=limit(16),
        cost_estimate=work(columns, sites, wraps),
        name="chain",
    )(arrived, hop, scale)


def add_up(offset, met, vertex, turned, total=None):
    _, width, columns = met.shape
    sites = vertex.shape[0]
    extra = [] if total is None else [total]
    return pl.pallas_call(
        functools.partial(add_kernel, offset, len(extra)),
        out_shape=jax.ShapeDtypeStruct((sites, width), jnp.float32),
        in_specs=[VMEM] * (2 + len(extra) + len(turned)),
        out_specs=VMEM,
        compiler_params=limit(16),
        cost_estimate=work(columns, sites, 1),
    )(met, vertex, *extra, *turned)


def fold(hop, scale, width):
    sites = hop.shape[0]
    return pl.pallas_call(
        fold_kernel,
        out_shape=jax.ShapeDtypeStruct((width, sites), jnp.bfloat16),
        in_specs=[VMEM] * 2,
        out_specs=VMEM,
        compiler_params=limit(16),
        cost_estimate=work(width, sites, 1),
        name="fold",
    )(hop, scale)


def finish(offset, ours, theirs, hop, folded, columns, vertex, total, turned):
    sites, width = total.shape
    blocks = 2
    return pl.pallas_call(
        functools.partial(finish_kernel, offset),
        out_shape=jax.ShapeDtypeStruct((sites, width), jnp.bfloat16),
        in_specs=[VMEM] * (7 + len(turned)),
        out_specs=HBM,
        scratch_shapes=[
            pltpu.VMEM((sites, width), jnp.bfloat16),
            pltpu.SemaphoreType.DMA((blocks,)),
        ],
        compiler_params=limit(16),
        cost_estimate=work(2 * ours.shape[1], sites, columns.shape[0]),
        name="finish",
    )(ours, theirs, hop, folded, columns, vertex, total, *turned)


def fetch_lines(lines):
    rows, count = lax.axis_size("rowt"), lines.shape[0]
    sites = lax.axis_size("site")
    if rows == count and rows & (rows - 1) == 0:
        bit = 1
        while bit < rows:
            pairs = [
                (i * sites + core, (i ^ bit) * sites + sites - 1 - core)
                for i in range(rows)
                for core in range(sites)
            ]
            came = lax.ppermute(lines, ("rowt", "site"), pairs)
            bit *= 2
            if bit < rows:
                lines = join(lines, came)
        return [lines, came], True
    found = []
    for step in range(count):
        line, shift = lines[step : step + 1], (step + 1) % rows
        if shift:
            line = lax.ppermute(line, "rowt", [((i + shift) % rows, i) for i in range(rows)])
        found.append(line)
    return found, False


def per_device(seed_green, field_spins, hop_matrix, vertex):
    cols, sites = lax.axis_size("colt"), lax.axis_size("site")
    wraps, width = field_spins.shape[0], seed_green.shape[-1]
    edge = width - LANES
    across = [
        (i * sites + core, (i + cols // 2) % cols * sites + sites - 1 - core)
        for i in range(cols)
        for core in range(sites)
    ]
    swap = [(i, sites - 1 - i) for i in range(sites)]

    pieces, lines = cut(seed_green[0, 0], field_spins, [(0, edge), (edge, width)])
    first = lax.ppermute(pieces[0], ("colt", "site"), across)
    second = lax.ppermute(pieces[1], ("colt", "site"), across)
    found, doubled = fetch_lines(hold(lines))
    hop, high_t, low_t, seed_t = prepare(hop_matrix, pieces)
    image = lift(seed_t, high_t, low_t, vertex)
    early, image, scale, columns = start_own(wraps, image, high_t, low_t, found, doubled)
    own = (high_t, low_t, scale)
    middle, level = propagate(1, 2, image, *own)
    keep, send = chain(first, hop, columns, width)
    came = lax.ppermute(send, "site", swap)
    (rest,) = propagate(2, wraps, level, *own)
    other = lax.ppermute(second, "site", swap)
    turned = [early, middle, rest]
    total = add_up(0, keep, vertex, turned)
    folded = fold(hop, scale, width)
    total = add_up(0, came, vertex, turned, total)
    result = finish(edge, second, other, hop, folded, columns, vertex, total, turned)
    return result[None, None]


def solution(mesh):
    return jax.shard_map(
        per_device,
        mesh=mesh,
        in_specs=(
            P(("groups", "rowt"), "colt", None, "site"),
            P(None, ("groups", "rowt"), None),
            P(),
            P(),
        ),
        out_specs=P(("groups", "rowt"), "colt", None, "site"),
        check_vma=False,
    )
```

```python
import functools

import jax
import jax.numpy as jnp
from jax import lax
from jax.experimental import pallas as pl
from jax.experimental.pallas import tpu as pltpu
from jax.sharding import PartitionSpec as P


coupling = 0.45
keep_share = 0.8
hop_share = 0.3
LANES = 128
PIECES = 4


VMEM = pl.BlockSpec(memory_space=pltpu.VMEM)
HBM = pl.BlockSpec(memory_space=pltpu.HBM)


def limit(mebibytes):
    return pltpu.CompilerParams(vmem_limit_bytes=mebibytes << 20)


def in_hbm(array):
    return pltpu.with_memory_space_constraint(array, pltpu.HBM)


def split_halves(value):
    high = value.astype(jnp.bfloat16)
    low = (value - high.astype(jnp.float32)).astype(jnp.bfloat16)
    return high, low


def site_spans(width):
    site = lax.axis_index("site")
    places = (site, lax.axis_size("site") - 1 - site)
    return [pl.ds(pl.multiple_of(place * width, LANES), width) for place in places]


def cut_kernel(seed_ref, piece, sems):
    width = seed_ref.shape[1]
    copies = []
    for half, source in enumerate(reversed(site_spans(width))):
        copy = pltpu.make_async_copy(
            seed_ref.at[source, pl.ds(0, piece.shape[1])],
            piece.at[pl.ds(half * width, width)],
            sems.at[half],
        )
        copy.start()
        copies.append(copy)
    for copy in copies:
        copy.wait()


def hold_kernel(spins_ref, seed_ref, lines_out, piece_out):
    lines = [spins_ref[step] for step in range(lines_out.shape[0])]
    lines_out[...] = jnp.concatenate(lines, axis=0).astype(jnp.float32).astype(jnp.bfloat16)
    width = seed_ref.shape[1]
    for half, source in enumerate(reversed(site_spans(width))):
        span = slice(half * width, (half + 1) * width)
        piece_out[span, :] = seed_ref[source, width - piece_out.shape[1] :]


def prepare_kernel(hop_ref, *refs):
    pieces = refs[:-4]
    hop_out, high_t, low_t, turned_out = refs[-4:]
    width, _ = turned_out.shape
    start = 0
    for piece in pieces:
        lines = slice(start, start + piece.shape[1])
        turned_out[lines, :width] = piece[width:, :].T
        turned_out[lines, width:] = piece[:width, :].T
        start += piece.shape[1]
    site = lax.axis_index("site")
    places = (site, lax.axis_size("site") - 1 - site)
    for half, place in enumerate(places):
        for start in range(0, width, LANES):
            rows = pl.ds(pl.multiple_of(place * width + start, LANES), LANES)
            strip = jnp.concatenate([hop_ref[rows, span] for span in site_spans(width)], axis=1)
            high, low = split_halves(hop_share * strip)
            spot = slice(half * width + start, half * width + start + LANES)
            hop_out[spot, :] = high
            high_t[:, spot] = high.T
            low_t[:, spot] = low.T


def hop_turned(narrow, high_t, low_t):
    hopped = jnp.dot(narrow, high_t[...], preferred_element_type=jnp.float32)
    if low_t is not None:
        hopped += jnp.dot(narrow, low_t[...], preferred_element_type=jnp.float32)
    return hopped


def lift_kernel(seed_t, high_t, low_t, _, image_out):
    narrow = seed_t[...]
    hopped = hop_turned(narrow, high_t, low_t)
    image_out[...] = keep_share * narrow.astype(jnp.float32) + hopped


def join_kernel(held_ref, came_ref, out_ref):
    out_ref[...] = jnp.concatenate([held_ref[...], came_ref[...]], axis=0)


def early_kernel(row_count, doubled, image_ref, high_t, low_t, *refs):
    *line_refs, turned_out, image_out, scale_out, column_out = refs
    wraps = scale_out.shape[0]
    row_index = lax.axis_index("rowt")
    lines = jnp.concatenate([ref[...].astype(jnp.float32) for ref in line_refs], axis=0)
    places = lax.broadcasted_iota(jnp.int32, lines.shape, 0)
    half = lines.shape[1] // 2
    other = jnp.concatenate([lines[:, half:], lines[:, :half]], axis=1)
    lines = jnp.where(lax.axis_index("site") == 0, lines, other)
    scales = []
    for step in range(wraps):
        target = (row_index + step + 1) % row_count
        if doubled:
            pick = (row_index ^ target) * wraps + step
            spins = jnp.sum(jnp.where(places == pick, lines, 0.0), axis=0, keepdims=True)
        else:
            spins = lines[step : step + 1]
        sign = jnp.where(target == 0, -1.0, 1.0)
        scales.append(sign * jnp.exp(coupling * (2.0 * spins - 1.0)))
    turned = scales[0] * image_ref[...]
    narrow = turned.astype(jnp.bfloat16)
    turned_out[0] = narrow
    image_out[...] = keep_share * turned + hop_turned(narrow, high_t, low_t)
    scale = jnp.concatenate(scales, axis=0)
    scale_out[...] = scale
    columns = scale.T
    for step in range(wraps):
        column_out[step] = jnp.broadcast_to(columns[:, step : step + 1], column_out.shape[1:])


def own_kernel(first, image_ref, high_t, low_t, scale_ref, turned_out, *rest):
    steps, wraps = turned_out.shape[0], scale_ref.shape[0]
    image = image_ref[...]
    for step in range(first, first + steps):
        turned = scale_ref[step : step + 1, :] * image
        narrow = turned.astype(jnp.bfloat16)
        turned_out[step - first] = narrow
        if step < wraps - 1:
            low = low_t if step < wraps - 2 else None
            image = keep_share * turned + hop_turned(narrow, high_t, low)
    if rest:
        rest[0][...] = image


def spread(columns, pieces):
    size = columns.shape[0] // pieces
    starts = range(0, columns.shape[0], size)
    return [columns[start : start + size].astype(jnp.float32) for start in starts]


def advance(step, halves, hop_ref, scale_ref, level, narrow):
    size, copies = level[0].shape[0], level[0].shape[1] // LANES
    source = jnp.concatenate(narrow, axis=0)
    new, fresh = [], []
    each = len(level) // 2
    for half in range(halves):
        for number in range(half * each, half * each + each):
            span = slice(number * size, (number + 1) * size)
            hopped = jnp.dot(hop_ref[span, :], source, preferred_element_type=jnp.float32)
            scale = jnp.concatenate([scale_ref[step, span, :]] * copies, axis=1)
            moved = scale * (keep_share * level[number] + hopped)
            new.append(moved)
            fresh.append(moved.astype(jnp.bfloat16))
        yield jnp.concatenate(fresh[half * each : half * each + each], axis=0)
    level[: len(new)] = new
    if halves == 2:
        narrow[:] = fresh


def chain_kernel(arrived, hop_ref, scale_ref, keep_out, send_out):
    level = spread(arrived[...], PIECES)
    narrow = [block.astype(jnp.bfloat16) for block in level]
    for step in range(keep_out.shape[0]):
        rounded = advance(step, 2, hop_ref, scale_ref, level, narrow)
        for value, out in zip(rounded, (keep_out, send_out)):
            out[step] = value


def multiply(met, own):
    return (met * own).astype(jnp.float32)


def own_levels(turned_refs, spans):
    for turned_ref in turned_refs:
        for step in range(turned_ref.shape[0]):
            parts = [turned_ref[step, :, span] for span in spans]
            yield parts[0] if len(parts) == 1 else jnp.concatenate(parts, axis=1)


def columns_at(offset, part, width):
    site = lax.axis_index("site")
    places = (lax.axis_size("site") - 1 - site, site)
    held = [slice(width + offset, width + offset + part), slice(offset, offset + part)]
    return held, [pl.ds(pl.multiple_of(p * width + offset, LANES), part) for p in places]


def against(corner, product):
    return lax.dot_general(
        corner, product, (((1,), (1,)), ((), ())), preferred_element_type=jnp.float32
    )


def sum_part(offset, which, met_ref, vertex_ref, turned_refs):
    _, width, part = met_ref.shape
    held, spots = columns_at(offset, part, width)
    pairs = None
    for step, own in enumerate(own_levels(turned_refs, [held[which]])):
        product = multiply(met_ref[step], own)
        pairs = product if pairs is None else pairs + product
    corner = vertex_ref[:, spots[which]]
    high, low = split_halves(pairs)
    return against(corner, high) + against(corner, low)


def add_kernel(offset, which, met_ref, vertex_ref, *refs):
    *turned_refs, out_ref = refs
    total = turned_refs.pop(0)[...] if which else 0.0
    out_ref[...] = total + sum_part(offset, which, met_ref, vertex_ref, turned_refs)


def fold_kernel(hop_ref, scale_ref, fold_out):
    width, wraps = fold_out.shape[0], scale_ref.shape[0]
    left = hop_ref[:width, :].astype(jnp.float32) * scale_ref[wraps - 2 : wraps - 1, :]
    right = jnp.dot(
        left.astype(jnp.bfloat16), hop_ref[...], preferred_element_type=jnp.float32
    )
    fold_out[...] = (keep_share * left + right).astype(jnp.bfloat16)


def finish_kernel(offset, *refs):
    ours, theirs, hop_ref, fold_ref, scale_ref, vertex_ref, total_ref, *turned_refs = refs[:-3]
    out_ref, result, sems = refs[-3:]
    wraps, (sites, width) = scale_ref.shape[0], total_ref.shape
    spans = [slice(0, width), slice(width, 2 * width)]
    held, spots = columns_at(offset, ours.shape[1], width)
    other = jnp.concatenate([theirs[span, :] for span in reversed(spans)], axis=0)
    level = spread(jnp.concatenate([ours[...], other], axis=1), PIECES)
    narrow = [block.astype(jnp.bfloat16) for block in level]
    pairs = None
    for step, own in enumerate(own_levels(turned_refs, held)):
        if step < wraps - 2:
            met, *_ = advance(step, 2, hop_ref, scale_ref, level, narrow)
        else:
            weights = hop_ref if step == wraps - 2 else fold_ref
            met, *_ = advance(step, 1, weights, scale_ref, level, narrow)
        product = multiply(met, own)
        pairs = product if pairs is None else pairs + product
    summed = pairs.astype(jnp.bfloat16)
    edges = [0, sites // 3, 2 * sites // 3, sites]
    copies = []
    for block, (begin, end) in enumerate(zip(edges, edges[1:])):
        span = slice(begin, end)
        corner = jnp.concatenate([vertex_ref[span, spot] for spot in spots], axis=1)
        total = total_ref[span, :] + against(corner, summed)
        result[span, :] = (total / wraps).astype(result.dtype)
        copy = pltpu.make_async_copy(
            result.at[pl.ds(begin, end - begin)],
            out_ref.at[pl.ds(begin, end - begin)],
            sems.at[block],
        )
        copy.start()
        copies.append(copy)
    for copy in copies:
        copy.wait()


def cut(seed, columns):
    return pl.pallas_call(
        cut_kernel,
        out_shape=jax.ShapeDtypeStruct((seed.shape[0], columns), jnp.bfloat16),
        in_specs=[HBM],
        out_specs=VMEM,
        scratch_shapes=[pltpu.SemaphoreType.DMA((2,))],
        compiler_params=limit(8),
        cost_estimate=pl.CostEstimate(flops=1 << 30, bytes_accessed=1 << 20, transcendentals=0),
        name="cut",
    )(in_hbm(seed))


def hold(spins, seed, columns):
    return pl.pallas_call(
        hold_kernel,
        out_shape=[
            jax.ShapeDtypeStruct((spins.shape[0], spins.shape[2]), jnp.bfloat16),
            jax.ShapeDtypeStruct((seed.shape[0], columns), jnp.bfloat16),
        ],
        in_specs=[VMEM] * 2,
        out_specs=[VMEM] * 2,
        compiler_params=limit(4),
        cost_estimate=pl.CostEstimate(flops=1 << 32, bytes_accessed=1 << 24, transcendentals=0),
        name="hold",
    )(spins, seed)


def prepare(hop_matrix, pieces):
    sites = hop_matrix.shape[0]
    width = sum(piece.shape[1] for piece in pieces)
    square = jax.ShapeDtypeStruct((sites, sites), jnp.bfloat16)
    return pl.pallas_call(
        prepare_kernel,
        out_shape=[square] * 3 + [jax.ShapeDtypeStruct((width, sites), jnp.bfloat16)],
        in_specs=[VMEM] * (1 + len(pieces)),
        out_specs=[VMEM] * 4,
        compiler_params=limit(8),
        cost_estimate=pl.CostEstimate(flops=1 << 28, bytes_accessed=1 << 22, transcendentals=0),
        name="prepare",
    )(hop_matrix, *pieces)


def lift(seed_t, high_t, low_t, vertex):
    width, sites = seed_t.shape
    return pl.pallas_call(
        lift_kernel,
        out_shape=jax.ShapeDtypeStruct((width, sites), jnp.float32),
        in_specs=[VMEM] * 4,
        out_specs=VMEM,
        compiler_params=limit(16),
        cost_estimate=work(width, sites, 2),
        name="lift",
    )(seed_t, high_t, low_t, vertex)


def join(held, came):
    shape = (held.shape[0] + came.shape[0], held.shape[1])
    return pl.pallas_call(
        join_kernel,
        out_shape=jax.ShapeDtypeStruct(shape, held.dtype),
        in_specs=[VMEM] * 2,
        out_specs=VMEM,
        compiler_params=limit(4),
        name="join",
    )(held, came)


def start_own(wraps, image, high_t, low_t, lines, doubled):
    width, sites = image.shape
    return pl.pallas_call(
        functools.partial(early_kernel, lax.axis_size("rowt"), doubled),
        out_shape=[
            jax.ShapeDtypeStruct((1, width, sites), jnp.bfloat16),
            jax.ShapeDtypeStruct((width, sites), jnp.float32),
            jax.ShapeDtypeStruct((wraps, sites), jnp.float32),
            jax.ShapeDtypeStruct((wraps, sites, LANES), jnp.float32),
        ],
        in_specs=[VMEM] * (3 + len(lines)),
        out_specs=[VMEM] * 4,
        compiler_params=limit(16),
        cost_estimate=work(width, sites, 2),
        name="early",
    )(image, high_t, low_t, *lines)


def propagate(first, last, image, high_t, low_t, scale):
    (width, sites), wraps = image.shape, scale.shape[0]
    outs = [jax.ShapeDtypeStruct((last - first, width, sites), jnp.bfloat16)]
    if last < wraps:
        outs.append(jax.ShapeDtypeStruct((width, sites), jnp.float32))
    return pl.pallas_call(
        functools.partial(own_kernel, first),
        out_shape=outs,
        in_specs=[VMEM] * 4,
        out_specs=[VMEM] * len(outs),
        compiler_params=limit(16),
        cost_estimate=work(width, sites, 2 * (last - first)),
    )(image, high_t, low_t, scale)


def work(columns, sites, wraps):
    return pl.CostEstimate(
        flops=wraps * sites * sites * columns // 16, bytes_accessed=1 << 16, transcendentals=0
    )


def chain(arrived, hop, scale, width):
    sites, columns = arrived.shape
    wraps = scale.shape[0]
    shape = jax.ShapeDtypeStruct((wraps, width, columns), jnp.bfloat16)
    return pl.pallas_call(
        chain_kernel,
        out_shape=[shape] * 2,
        in_specs=[VMEM] * 3,
        out_specs=[VMEM] * 2,
        compiler_params=limit(16),
        cost_estimate=work(columns, sites, wraps),
        name="chain",
    )(arrived, hop, scale)


def add_up(offset, met, vertex, turned, total=None):
    _, width, columns = met.shape
    sites = vertex.shape[0]
    extra = [] if total is None else [total]
    return pl.pallas_call(
        functools.partial(add_kernel, offset, len(extra)),
        out_shape=jax.ShapeDtypeStruct((sites, width), jnp.float32),
        in_specs=[VMEM] * (2 + len(extra) + len(turned)),
        out_specs=VMEM,
        compiler_params=limit(16),
        cost_estimate=work(columns, sites, 1),
    )(met, vertex, *extra, *turned)


def fold(hop, scale, width):
    sites = hop.shape[0]
    return pl.pallas_call(
        fold_kernel,
        out_shape=jax.ShapeDtypeStruct((width, sites), jnp.bfloat16),
        in_specs=[VMEM] * 2,
        out_specs=VMEM,
        compiler_params=limit(16),
        cost_estimate=work(width, sites, 1),
        name="fold",
    )(hop, scale)


def finish(offset, ours, theirs, hop, folded, columns, vertex, total, turned):
    sites, width = total.shape
    blocks = 3
    return pl.pallas_call(
        functools.partial(finish_kernel, offset),
        out_shape=jax.ShapeDtypeStruct((sites, width), jnp.bfloat16),
        in_specs=[VMEM] * (7 + len(turned)),
        out_specs=HBM,
        scratch_shapes=[
            pltpu.VMEM((sites, width), jnp.bfloat16),
            pltpu.SemaphoreType.DMA((blocks,)),
        ],
        compiler_params=limit(16),
        cost_estimate=work(2 * ours.shape[1], sites, columns.shape[0]),
        name="finish",
    )(ours, theirs, hop, folded, columns, vertex, total, *turned)


def fetch_lines(lines):
    rows, count = lax.axis_size("rowt"), lines.shape[0]
    sites = lax.axis_size("site")
    if rows == count and rows & (rows - 1) == 0:
        bit = 1
        while bit < rows:
            pairs = [
                (i * sites + core, (i ^ bit) * sites + sites - 1 - core)
                for i in range(rows)
                for core in range(sites)
            ]
            came = lax.ppermute(lines, ("rowt", "site"), pairs)
            bit *= 2
            if bit < rows:
                lines = join(lines, came)
        return [lines, came], True
    found = []
    for step in range(count):
        line, shift = lines[step : step + 1], (step + 1) % rows
        if shift:
            line = lax.ppermute(line, "rowt", [((i + shift) % rows, i) for i in range(rows)])
        found.append(line)
    return found, False


def per_device(seed_green, field_spins, hop_matrix, vertex):
    cols, sites = lax.axis_size("colt"), lax.axis_size("site")
    wraps, width = field_spins.shape[0], seed_green.shape[-1]
    edge = width - LANES
    across = [
        (i * sites + core, (i + cols // 2) % cols * sites + sites - 1 - core)
        for i in range(cols)
        for core in range(sites)
    ]
    swap = [(i, sites - 1 - i) for i in range(sites)]

    seed = seed_green[0, 0]
    pieces = [cut(seed, edge)]
    first = lax.ppermute(pieces[0], ("colt", "site"), across)
    lines, piece = hold(field_spins, seed, width - edge)
    pieces.append(piece)
    second = lax.ppermute(piece, ("colt", "site"), across)
    found, doubled = fetch_lines(lines)
    hop, high_t, low_t, seed_t = prepare(hop_matrix, pieces)
    image = lift(seed_t, high_t, low_t, vertex)
    early, image, scale, columns = start_own(wraps, image, high_t, low_t, found, doubled)
    own = (high_t, low_t, scale)
    middle, level = propagate(1, 2, image, *own)
    keep, send = chain(first, hop, columns, width)
    came = lax.ppermute(send, "site", swap)
    (rest,) = propagate(2, wraps, level, *own)
    other = lax.ppermute(second, "site", swap)
    turned = [early, middle, rest]
    total = add_up(0, keep, vertex, turned)
    folded = fold(hop, scale, width)
    total = add_up(0, came, vertex, turned, total)
    result = finish(edge, second, other, hop, folded, columns, vertex, total, turned)
    return result[None, None]


def solution(mesh):
    return jax.shard_map(
        per_device,
        mesh=mesh,
        in_specs=(
            P(("groups", "rowt"), "colt", None, "site"),
            P(None, ("groups", "rowt"), None),
            P(),
            P(),
        ),
        out_specs=P(("groups", "rowt"), "colt", None, "site"),
        check_vma=False,
    )
```

```python
import functools

import jax
import jax.numpy as jnp
from jax import lax
from jax.experimental import pallas as pl
from jax.experimental.pallas import tpu as pltpu
from jax.sharding import PartitionSpec as P


coupling = 0.45
keep_share = 0.8
hop_share = 0.3
LANES = 128
PIECES = 4


VMEM = pl.BlockSpec(memory_space=pltpu.VMEM)
HBM = pl.BlockSpec(memory_space=pltpu.HBM)


def limit(mebibytes):
    return pltpu.CompilerParams(vmem_limit_bytes=mebibytes << 20)


def in_hbm(array):
    return pltpu.with_memory_space_constraint(array, pltpu.HBM)


def split_halves(value):
    high = value.astype(jnp.bfloat16)
    low = (value - high.astype(jnp.float32)).astype(jnp.bfloat16)
    return high, low


def site_spans(width):
    site = lax.axis_index("site")
    places = (site, lax.axis_size("site") - 1 - site)
    return [pl.ds(pl.multiple_of(place * width, LANES), width) for place in places]


def cut_kernel(seed_ref, piece, sems):
    width = seed_ref.shape[1]
    copies = []
    for half, source in enumerate(reversed(site_spans(width))):
        copy = pltpu.make_async_copy(
            seed_ref.at[source, pl.ds(0, piece.shape[1])],
            piece.at[pl.ds(half * width, width)],
            sems.at[half],
        )
        copy.start()
        copies.append(copy)
    for copy in copies:
        copy.wait()


def hold_kernel(spins_ref, seed_ref, lines_out, piece_out):
    lines = [spins_ref[step] for step in range(lines_out.shape[0])]
    lines_out[...] = jnp.concatenate(lines, axis=0).astype(jnp.float32).astype(jnp.bfloat16)
    width = seed_ref.shape[1]
    for half, source in enumerate(reversed(site_spans(width))):
        span = slice(half * width, (half + 1) * width)
        piece_out[span, :] = seed_ref[source, width - piece_out.shape[1] :]


def prepare_kernel(hop_ref, *refs):
    pieces = refs[:-4]
    hop_out, high_t, low_t, turned_out = refs[-4:]
    width, _ = turned_out.shape
    start = 0
    for piece in pieces:
        lines = slice(start, start + piece.shape[1])
        turned_out[lines, :width] = piece[width:, :].T
        turned_out[lines, width:] = piece[:width, :].T
        start += piece.shape[1]
    site = lax.axis_index("site")
    places = (site, lax.axis_size("site") - 1 - site)
    for half, place in enumerate(places):
        for start in range(0, width, LANES):
            rows = pl.ds(pl.multiple_of(place * width + start, LANES), LANES)
            strip = jnp.concatenate([hop_ref[rows, span] for span in site_spans(width)], axis=1)
            high, low = split_halves(hop_share * strip)
            spot = slice(half * width + start, half * width + start + LANES)
            hop_out[spot, :] = high
            high_t[:, spot] = high.T
            low_t[:, spot] = low.T


def hop_turned(narrow, high_t, low_t):
    hopped = jnp.dot(narrow, high_t[...], preferred_element_type=jnp.float32)
    if low_t is not None:
        hopped += jnp.dot(narrow, low_t[...], preferred_element_type=jnp.float32)
    return hopped


def lift_kernel(seed_t, high_t, low_t, _, image_out):
    narrow = seed_t[...]
    hopped = hop_turned(narrow, high_t, low_t)
    image_out[...] = keep_share * narrow.astype(jnp.float32) + hopped


def join_kernel(held_ref, came_ref, out_ref):
    out_ref[...] = jnp.concatenate([held_ref[...], came_ref[...]], axis=0)


def early_kernel(row_count, doubled, image_ref, high_t, low_t, *refs):
    *line_refs, turned_out, image_out, scale_out, column_out = refs
    wraps = scale_out.shape[0]
    row_index = lax.axis_index("rowt")
    lines = jnp.concatenate([ref[...].astype(jnp.float32) for ref in line_refs], axis=0)
    places = lax.broadcasted_iota(jnp.int32, lines.shape, 0)
    half = lines.shape[1] // 2
    other = jnp.concatenate([lines[:, half:], lines[:, :half]], axis=1)
    lines = jnp.where(lax.axis_index("site") == 0, lines, other)
    scales = []
    for step in range(wraps):
        target = (row_index + step + 1) % row_count
        if doubled:
            pick = (row_index ^ target) * wraps + step
            spins = jnp.sum(jnp.where(places == pick, lines, 0.0), axis=0, keepdims=True)
        else:
            spins = lines[step : step + 1]
        sign = jnp.where(target == 0, -1.0, 1.0)
        scales.append(sign * jnp.exp(coupling * (2.0 * spins - 1.0)))
    image = image_ref[...]
    for step in range(turned_out.shape[0]):
        turned = scales[step] * image
        narrow = turned.astype(jnp.bfloat16)
        turned_out[step] = narrow
        image = keep_share * turned + hop_turned(narrow, high_t, low_t)
    image_out[...] = image
    scale = jnp.concatenate(scales, axis=0)
    scale_out[...] = scale
    columns = scale.T
    for step in range(wraps):
        column_out[step] = jnp.broadcast_to(columns[:, step : step + 1], column_out.shape[1:])


def own_kernel(first, image_ref, high_t, low_t, scale_ref, turned_out, *rest):
    steps, wraps = turned_out.shape[0], scale_ref.shape[0]
    image = image_ref[...]
    for step in range(first, first + steps):
        turned = scale_ref[step : step + 1, :] * image
        narrow = turned.astype(jnp.bfloat16)
        turned_out[step - first] = narrow
        if step < wraps - 1:
            low = low_t if step < wraps - 2 else None
            image = keep_share * turned + hop_turned(narrow, high_t, low)
    if rest:
        rest[0][...] = image


def spread(columns, pieces):
    size = columns.shape[0] // pieces
    starts = range(0, columns.shape[0], size)
    return [columns[start : start + size].astype(jnp.float32) for start in starts]


def advance(step, halves, hop_ref, scale_ref, level, narrow):
    size, copies = level[0].shape[0], level[0].shape[1] // LANES
    source = jnp.concatenate(narrow, axis=0)
    new, fresh = [], []
    each = len(level) // 2
    for half in range(halves):
        for number in range(half * each, half * each + each):
            span = slice(number * size, (number + 1) * size)
            hopped = jnp.dot(hop_ref[span, :], source, preferred_element_type=jnp.float32)
            scale = jnp.concatenate([scale_ref[step, span, :]] * copies, axis=1)
            moved = scale * (keep_share * level[number] + hopped)
            new.append(moved)
            fresh.append(moved.astype(jnp.bfloat16))
        yield jnp.concatenate(fresh[half * each : half * each + each], axis=0)
    level[: len(new)] = new
    if halves == 2:
        narrow[:] = fresh


def chain_kernel(arrived, hop_ref, scale_ref, keep_out, send_out):
    level = spread(arrived[...], PIECES)
    narrow = [block.astype(jnp.bfloat16) for block in level]
    for step in range(keep_out.shape[0]):
        rounded = advance(step, 2, hop_ref, scale_ref, level, narrow)
        for value, out in zip(rounded, (keep_out, send_out)):
            out[step] = value


def multiply(met, own):
    return (met * own).astype(jnp.float32)


def own_levels(turned_refs, spans):
    for turned_ref in turned_refs:
        for step in range(turned_ref.shape[0]):
            parts = [turned_ref[step, :, span] for span in spans]
            yield parts[0] if len(parts) == 1 else jnp.concatenate(parts, axis=1)


def columns_at(offset, part, width):
    site = lax.axis_index("site")
    places = (lax.axis_size("site") - 1 - site, site)
    held = [slice(width + offset, width + offset + part), slice(offset, offset + part)]
    return held, [pl.ds(pl.multiple_of(p * width + offset, LANES), part) for p in places]


def against(corner, product):
    return lax.dot_general(
        corner, product, (((1,), (1,)), ((), ())), preferred_element_type=jnp.float32
    )


def sum_part(offset, which, met_ref, vertex_ref, turned_refs):
    _, width, part = met_ref.shape
    held, spots = columns_at(offset, part, width)
    pairs = None
    for step, own in enumerate(own_levels(turned_refs, [held[which]])):
        product = multiply(met_ref[step], own)
        pairs = product if pairs is None else pairs + product
    corner = vertex_ref[:, spots[which]]
    high, low = split_halves(pairs)
    return against(corner, high) + against(corner, low)


def add_kernel(offset, which, met_ref, vertex_ref, *refs):
    *turned_refs, out_ref = refs
    total = turned_refs.pop(0)[...] if which else 0.0
    out_ref[...] = total + sum_part(offset, which, met_ref, vertex_ref, turned_refs)


def fold_kernel(hop_ref, scale_ref, fold_out):
    width, wraps = fold_out.shape[0], scale_ref.shape[0]
    left = hop_ref[:width, :].astype(jnp.float32) * scale_ref[wraps - 2 : wraps - 1, :]
    right = jnp.dot(
        left.astype(jnp.bfloat16), hop_ref[...], preferred_element_type=jnp.float32
    )
    fold_out[...] = (keep_share * left + right).astype(jnp.bfloat16)


def finish_kernel(offset, *refs):
    ours, theirs, hop_ref, fold_ref, scale_ref, vertex_ref, total_ref, *turned_refs = refs[:-3]
    out_ref, result, sems = refs[-3:]
    wraps, (sites, width) = scale_ref.shape[0], total_ref.shape
    spans = [slice(0, width), slice(width, 2 * width)]
    held, spots = columns_at(offset, ours.shape[1], width)
    other = jnp.concatenate([theirs[span, :] for span in reversed(spans)], axis=0)
    level = spread(jnp.concatenate([ours[...], other], axis=1), PIECES)
    narrow = [block.astype(jnp.bfloat16) for block in level]
    pairs = None
    for step, own in enumerate(own_levels(turned_refs, held)):
        if step < wraps - 2:
            met, *_ = advance(step, 2, hop_ref, scale_ref, level, narrow)
        else:
            weights = hop_ref if step == wraps - 2 else fold_ref
            met, *_ = advance(step, 1, weights, scale_ref, level, narrow)
        product = multiply(met, own)
        pairs = product if pairs is None else pairs + product
    summed = pairs.astype(jnp.bfloat16)
    edges = [0, sites // 3, 2 * sites // 3, sites]
    copies = []
    for block, (begin, end) in enumerate(zip(edges, edges[1:])):
        span = slice(begin, end)
        corner = jnp.concatenate([vertex_ref[span, spot] for spot in spots], axis=1)
        total = total_ref[span, :] + against(corner, summed)
        result[span, :] = (total / wraps).astype(result.dtype)
        copy = pltpu.make_async_copy(
            result.at[pl.ds(begin, end - begin)],
            out_ref.at[pl.ds(begin, end - begin)],
            sems.at[block],
        )
        copy.start()
        copies.append(copy)
    for copy in copies:
        copy.wait()


def cut(seed, columns):
    return pl.pallas_call(
        cut_kernel,
        out_shape=jax.ShapeDtypeStruct((seed.shape[0], columns), jnp.bfloat16),
        in_specs=[HBM],
        out_specs=VMEM,
        scratch_shapes=[pltpu.SemaphoreType.DMA((2,))],
        compiler_params=limit(8),
        cost_estimate=pl.CostEstimate(flops=1 << 30, bytes_accessed=1 << 20, transcendentals=0),
        name="cut",
    )(in_hbm(seed))


def hold(spins, seed, columns):
    return pl.pallas_call(
        hold_kernel,
        out_shape=[
            jax.ShapeDtypeStruct((spins.shape[0], spins.shape[2]), jnp.bfloat16),
            jax.ShapeDtypeStruct((seed.shape[0], columns), jnp.bfloat16),
        ],
        in_specs=[VMEM] * 2,
        out_specs=[VMEM] * 2,
        compiler_params=limit(4),
        cost_estimate=pl.CostEstimate(flops=1 << 32, bytes_accessed=1 << 24, transcendentals=0),
        name="hold",
    )(spins, seed)


def prepare(hop_matrix, pieces):
    sites = hop_matrix.shape[0]
    width = sum(piece.shape[1] for piece in pieces)
    square = jax.ShapeDtypeStruct((sites, sites), jnp.bfloat16)
    return pl.pallas_call(
        prepare_kernel,
        out_shape=[square] * 3 + [jax.ShapeDtypeStruct((width, sites), jnp.bfloat16)],
        in_specs=[VMEM] * (1 + len(pieces)),
        out_specs=[VMEM] * 4,
        compiler_params=limit(8),
        cost_estimate=pl.CostEstimate(flops=1 << 28, bytes_accessed=1 << 22, transcendentals=0),
        name="prepare",
    )(hop_matrix, *pieces)


def lift(seed_t, high_t, low_t, vertex):
    width, sites = seed_t.shape
    return pl.pallas_call(
        lift_kernel,
        out_shape=jax.ShapeDtypeStruct((width, sites), jnp.float32),
        in_specs=[VMEM] * 4,
        out_specs=VMEM,
        compiler_params=limit(16),
        cost_estimate=work(width, sites, 2),
        name="lift",
    )(seed_t, high_t, low_t, vertex)


def join(held, came):
    shape = (held.shape[0] + came.shape[0], held.shape[1])
    return pl.pallas_call(
        join_kernel,
        out_shape=jax.ShapeDtypeStruct(shape, held.dtype),
        in_specs=[VMEM] * 2,
        out_specs=VMEM,
        compiler_params=limit(4),
        name="join",
    )(held, came)


def start_own(wraps, image, high_t, low_t, lines, doubled):
    width, sites = image.shape
    return pl.pallas_call(
        functools.partial(early_kernel, lax.axis_size("rowt"), doubled),
        out_shape=[
            jax.ShapeDtypeStruct((wraps // 2, width, sites), jnp.bfloat16),
            jax.ShapeDtypeStruct((width, sites), jnp.float32),
            jax.ShapeDtypeStruct((wraps, sites), jnp.float32),
            jax.ShapeDtypeStruct((wraps, sites, LANES), jnp.float32),
        ],
        in_specs=[VMEM] * (3 + len(lines)),
        out_specs=[VMEM] * 4,
        compiler_params=limit(16),
        cost_estimate=work(width, sites, 2),
        name="early",
    )(image, high_t, low_t, *lines)


def propagate(first, last, image, high_t, low_t, scale):
    (width, sites), wraps = image.shape, scale.shape[0]
    outs = [jax.ShapeDtypeStruct((last - first, width, sites), jnp.bfloat16)]
    if last < wraps:
        outs.append(jax.ShapeDtypeStruct((width, sites), jnp.float32))
    return pl.pallas_call(
        functools.partial(own_kernel, first),
        out_shape=outs,
        in_specs=[VMEM] * 4,
        out_specs=[VMEM] * len(outs),
        compiler_params=limit(16),
        cost_estimate=work(width, sites, 2 * (last - first)),
    )(image, high_t, low_t, scale)


def work(columns, sites, wraps):
    return pl.CostEstimate(
        flops=wraps * sites * sites * columns // 16, bytes_accessed=1 << 16, transcendentals=0
    )


def chain(arrived, hop, scale, width):
    sites, columns = arrived.shape
    wraps = scale.shape[0]
    shape = jax.ShapeDtypeStruct((wraps, width, columns), jnp.bfloat16)
    return pl.pallas_call(
        chain_kernel,
        out_shape=[shape] * 2,
        in_specs=[VMEM] * 3,
        out_specs=[VMEM] * 2,
        compiler_params=limit(16),
        cost_estimate=work(columns, sites, wraps),
        name="chain",
    )(arrived, hop, scale)


def add_up(offset, met, vertex, turned, total=None):
    _, width, columns = met.shape
    sites = vertex.shape[0]
    extra = [] if total is None else [total]
    return pl.pallas_call(
        functools.partial(add_kernel, offset, len(extra)),
        out_shape=jax.ShapeDtypeStruct((sites, width), jnp.float32),
        in_specs=[VMEM] * (2 + len(extra) + len(turned)),
        out_specs=VMEM,
        compiler_params=limit(16),
        cost_estimate=work(columns, sites, 1),
    )(met, vertex, *extra, *turned)


def fold(hop, scale, width):
    sites = hop.shape[0]
    return pl.pallas_call(
        fold_kernel,
        out_shape=jax.ShapeDtypeStruct((width, sites), jnp.bfloat16),
        in_specs=[VMEM] * 2,
        out_specs=VMEM,
        compiler_params=limit(16),
        cost_estimate=work(width, sites, 1),
        name="fold",
    )(hop, scale)


def finish(offset, ours, theirs, hop, folded, columns, vertex, total, turned):
    sites, width = total.shape
    blocks = 3
    return pl.pallas_call(
        functools.partial(finish_kernel, offset),
        out_shape=jax.ShapeDtypeStruct((sites, width), jnp.bfloat16),
        in_specs=[VMEM] * (7 + len(turned)),
        out_specs=HBM,
        scratch_shapes=[
            pltpu.VMEM((sites, width), jnp.bfloat16),
            pltpu.SemaphoreType.DMA((blocks,)),
        ],
        compiler_params=limit(16),
        cost_estimate=work(2 * ours.shape[1], sites, columns.shape[0]),
        name="finish",
    )(ours, theirs, hop, folded, columns, vertex, total, *turned)


def fetch_lines(lines):
    rows, count = lax.axis_size("rowt"), lines.shape[0]
    sites = lax.axis_size("site")
    if rows == count and rows & (rows - 1) == 0:
        bit = 1
        while bit < rows:
            pairs = [
                (i * sites + core, (i ^ bit) * sites + sites - 1 - core)
                for i in range(rows)
                for core in range(sites)
            ]
            came = lax.ppermute(lines, ("rowt", "site"), pairs)
            bit *= 2
            if bit < rows:
                lines = join(lines, came)
        return [lines, came], True
    found = []
    for step in range(count):
        line, shift = lines[step : step + 1], (step + 1) % rows
        if shift:
            line = lax.ppermute(line, "rowt", [((i + shift) % rows, i) for i in range(rows)])
        found.append(line)
    return found, False


def per_device(seed_green, field_spins, hop_matrix, vertex):
    cols, sites = lax.axis_size("colt"), lax.axis_size("site")
    wraps, width = field_spins.shape[0], seed_green.shape[-1]
    edge = width - LANES
    across = [
        (i * sites + core, (i + cols // 2) % cols * sites + sites - 1 - core)
        for i in range(cols)
        for core in range(sites)
    ]
    swap = [(i, sites - 1 - i) for i in range(sites)]

    seed = seed_green[0, 0]
    pieces = [cut(seed, edge)]
    first = lax.ppermute(pieces[0], ("colt", "site"), across)
    lines, piece = hold(field_spins, seed, width - edge)
    pieces.append(piece)
    second = lax.ppermute(piece, ("colt", "site"), across)
    found, doubled = fetch_lines(lines)
    hop, high_t, low_t, seed_t = prepare(hop_matrix, pieces)
    image = lift(seed_t, high_t, low_t, vertex)
    early, image, scale, columns = start_own(wraps, image, high_t, low_t, found, doubled)
    own = (high_t, low_t, scale)
    keep, send = chain(first, hop, columns, width)
    came = lax.ppermute(send, "site", swap)
    (rest,) = propagate(wraps // 2, wraps, image, *own)
    other = lax.ppermute(second, "site", swap)
    turned = [early, rest]
    total = add_up(0, keep, vertex, turned)
    folded = fold(hop, scale, width)
    total = add_up(0, came, vertex, turned, total)
    result = finish(edge, second, other, hop, folded, columns, vertex, total, turned)
    return result[None, None]


def solution(mesh):
    return jax.shard_map(
        per_device,
        mesh=mesh,
        in_specs=(
            P(("groups", "rowt"), "colt", None, "site"),
            P(None, ("groups", "rowt"), None),
            P(),
            P(),
        ),
        out_specs=P(("groups", "rowt"), "colt", None, "site"),
        check_vma=False,
    )
```
